64 devices in a mesh: dp: 4 (over x, y), dpa: 16 (over z, core).
Axes of the slice: x: 2, y: 2, z: 8, core: 2. Of those that a mesh axis runs over, the one named last changes fastest.
The devices are a block of a 4x4x8 slice.
Arguments:
- x: bfloat16 [64, 1, 384, 2048], P(('dp', 'dpa')), parts along dimension 0
- chunk_len: int32 [64, 1], P(('dp', 'dpa')), parts along dimension 0
- ctx_len: int32 [64, 1], P(('dp', 'dpa')), parts along dimension 0
- lat_cache: bfloat16 [64, 1, 1024, 512], P(('dp', 'dpa')), parts along dimension 0
- rope_cache: bfloat16 [64, 1, 1024, 64], P(('dp', 'dpa')), parts along dimension 0
- topk_idx: int32 [64, 1, 384, 6], P(('dp', 'dpa')), parts along dimension 0
- g_attn: bfloat16 [2048], replicated
- w_q: bfloat16 [2048, 16, 192], replicated
- w_dkv: bfloat16 [2048, 512], replicated
- g_kv: bfloat16 [512], replicated
- w_kr: bfloat16 [2048, 64], replicated
- w_uk: bfloat16 [512, 16, 128], replicated
- w_uv: bfloat16 [512, 16, 128], replicated
- w_o: bfloat16 [16, 128, 2048], replicated
- g_ffn: bfloat16 [2048], replicated
- w_router: bfloat16 [2048, 64], replicated
- w_sh_gate: bfloat16 [2048, 2816], replicated
- w_sh_up: bfloat16 [2048, 2816], replicated
- w_sh_down: bfloat16 [2816, 2048], replicated
- w_exp_gate: bfloat16 [64, 2048, 1408], P('dpa')
- w_exp_up: bfloat16 [64, 2048, 1408], P('dpa')
- w_exp_down: bfloat16 [64, 1408, 2048], P('dpa')
Outputs:
- output 1: bfloat16 [64, 1, 384, 2048], P(('dp', 'dpa')), parts along dimension 0
- output 2: bfloat16 [64, 1, 1024, 512], P(('dp', 'dpa')), parts along dimension 0
- output 3: bfloat16 [64, 1, 1024, 64], P(('dp', 'dpa')), parts along dimension 0
There are 4 independent parts. The reference program is written for one: setup_inputs(seed, part) draws one part's arguments, and reference() takes and returns one part's arrays. A program takes and returns all parts, laid end to end along the dimension named above; an argument that names none is the same for every part.
All inputs are finite; a program needn't handle non-finite values.
Results may differ from the reference program's by a relative error of at most 0.0196086.
Values are sent between devices in bfloat16 or wider.
A program may use at most 768 MiB of HBM per device.

```python
import jax
import jax.numpy as jnp
from jax import lax

GROUP = 16
REQS = 1
CHUNK = 384
CTX = 1024
HID = 2048
HEADS = 16
NOPE = 128
ROPE = 64
VDIM = 128
RANK = 512
EXPERTS = 64
EXP_FF = 1408
SHARED_FF = 2816
TOP = 6
BLOCK_ROWS = 128

TOKENS = REQS * CHUNK
LOCAL = EXPERTS // GROUP
QDIM = NOPE + ROPE
EPS = 1e-6
THETA = 10000.0


def draw_normal(rand_key, shape, scale):
    return (jax.random.normal(rand_key, shape, jnp.float32) * scale).astype(jnp.bfloat16)


def draw_gain(rand_key, width):
    return jax.random.uniform(rand_key, (width,), jnp.float32, 0.5, 1.5).astype(jnp.bfloat16)


def draw_lengths(rand_key):
    chunk_key, ctx_key = jax.random.split(rand_key)
    chunk_len = jax.random.randint(chunk_key, (GROUP, REQS), CHUNK // 4, CHUNK + 1).astype(jnp.int32)
    ctx_len = jax.random.randint(ctx_key, (GROUP, REQS), CTX // 8, CTX - CHUNK + 1).astype(jnp.int32)
    return chunk_len.at[0, 0].set(CHUNK), ctx_len.at[GROUP - 1, REQS - 1].set(CTX - CHUNK)


def draw_routes(rand_key):
    start_key, local_key = jax.random.split(rand_key)
    shuffled = jax.vmap(lambda sub_key: jax.random.permutation(sub_key, TOKENS))(jax.random.split(start_key, GROUP))
    first_dev = shuffled % GROUP
    first_loc = jax.random.randint(local_key, (GROUP, TOKENS), 0, LOCAL)
    slot_ids = jnp.arange(TOP)
    target = (first_dev[:, :, None] + slot_ids) % GROUP
    local_id = (first_loc[:, :, None] + slot_ids // GROUP) % LOCAL
    return (target * LOCAL + local_id).reshape(GROUP, REQS, CHUNK, TOP).astype(jnp.int32)


def setup_inputs(seed: int = 0, part: int = 0) -> dict:
    base_key = jax.random.key(seed)
    part_keys = jax.random.split(jax.random.fold_in(base_key, part), 6)
    shared_keys = jax.random.split(base_key, 16)
    chunk_len, ctx_len = draw_lengths(part_keys[0])
    return {
        'x': draw_normal(part_keys[1], (GROUP, REQS, CHUNK, HID), 1.0),
        'chunk_len': chunk_len,
        'ctx_len': ctx_len,
        'lat_cache': draw_normal(part_keys[2], (GROUP, REQS, CTX, RANK), 1.0),
        'rope_cache': draw_normal(part_keys[3], (GROUP, REQS, CTX, ROPE), 1.0),
        'topk_idx': draw_routes(part_keys[4]),
        'g_attn': draw_gain(shared_keys[0], HID),
        'w_q': draw_normal(shared_keys[1], (HID, HEADS, QDIM), HID ** -0.5),
        'w_dkv': draw_normal(shared_keys[2], (HID, RANK), HID ** -0.5),
        'g_kv': draw_gain(shared_keys[3], RANK),
        'w_kr': draw_normal(shared_keys[4], (HID, ROPE), HID ** -0.5),
        'w_uk': draw_normal(shared_keys[5], (RANK, HEADS, NOPE), 2.5 * NOPE ** -0.5),
        'w_uv': draw_normal(shared_keys[6], (RANK, HEADS, VDIM), RANK ** -0.5),
        'w_o': draw_normal(shared_keys[7], (HEADS, VDIM, HID), 4.0 * (HEADS * VDIM) ** -0.5),
        'g_ffn': draw_gain(shared_keys[8], HID),
        'w_router': draw_normal(shared_keys[9], (HID, EXPERTS), HID ** -0.5),
        'w_sh_gate': draw_normal(shared_keys[10], (HID, SHARED_FF), HID ** -0.5),
        'w_sh_up': draw_normal(shared_keys[11], (HID, SHARED_FF), HID ** -0.5),
        'w_sh_down': draw_normal(shared_keys[12], (SHARED_FF, HID), SHARED_FF ** -0.5),
        'w_exp_gate': draw_normal(shared_keys[13], (EXPERTS, HID, EXP_FF), HID ** -0.5),
        'w_exp_up': draw_normal(shared_keys[14], (EXPERTS, HID, EXP_FF), HID ** -0.5),
        'w_exp_down': draw_normal(shared_keys[15], (EXPERTS, EXP_FF, HID), 0.8 * EXPERTS * EXP_FF ** -0.5),
    }


def rms_norm(vals, gain):
    vals_f32 = vals.astype(jnp.float32)
    inv_rms = lax.rsqrt(jnp.mean(vals_f32 * vals_f32, axis=-1, keepdims=True) + EPS)
    return (vals_f32 * inv_rms * gain.astype(jnp.float32)).astype(jnp.bfloat16)


def rope_tables(positions):
    inv_freq = THETA ** (-2.0 * jnp.arange(ROPE // 2, dtype=jnp.float32) / ROPE)
    angle = positions.astype(jnp.float32)[..., None] * inv_freq
    return jnp.cos(angle), jnp.sin(angle)


def rotate(vals, cos_tab, sin_tab):
    half = ROPE // 2
    first = vals[..., :half]
    second = vals[..., half:]
    return jnp.concatenate([first * cos_tab - second * sin_tab, second * cos_tab + first * sin_tab], axis=-1)


def write_window(cache_row, new_rows, start, keep):
    old_rows = lax.dynamic_slice_in_dim(cache_row, start, CHUNK, axis=0)
    merged = jnp.where(keep[:, None], new_rows, old_rows)
    return lax.dynamic_update_slice_in_dim(cache_row, merged, start, axis=0)


def reference(x, chunk_len, ctx_len, lat_cache, rope_cache, topk_idx, g_attn, w_q, w_dkv, g_kv, w_kr, w_uk, w_uv, w_o, g_ffn, w_router, w_sh_gate, w_sh_up, w_sh_down, w_exp_gate, w_exp_up, w_exp_down):
    def one_request(args):
        x_req, req_chunk, req_ctx, lat_old, rope_old = args
        normed = rms_norm(x_req, g_attn)
        q_full = jnp.dot(normed, w_q.reshape(HID, HEADS * QDIM), preferred_element_type=jnp.float32).astype(jnp.bfloat16).reshape(CHUNK, HEADS, QDIM)
        positions = req_ctx + jnp.arange(CHUNK)
        cos_tab, sin_tab = rope_tables(positions)
        q_rope = rotate(q_full[:, :, NOPE:].astype(jnp.float32), cos_tab[:, None, :], sin_tab[:, None, :]).astype(jnp.bfloat16)
        q_lat = jnp.einsum('chn,khn->chk', q_full[:, :, :NOPE].astype(jnp.float32), w_uk.astype(jnp.float32)).astype(jnp.bfloat16)
        lat_new = rms_norm(jnp.dot(normed, w_dkv, preferred_element_type=jnp.float32), g_kv)
        rope_new = rotate(jnp.dot(normed, w_kr, preferred_element_type=jnp.float32), cos_tab, sin_tab).astype(jnp.bfloat16)
        keep = jnp.arange(CHUNK) < req_chunk
        lat_upd = write_window(lat_old, lat_new, req_ctx, keep)
        rope_upd = write_window(rope_old, rope_new, req_ctx, keep)
        lat_f32 = lat_upd.astype(jnp.float32)
        scores = (jnp.einsum('chk,lk->chl', q_lat.astype(jnp.float32), lat_f32) + jnp.einsum('chp,lp->chl', q_rope.astype(jnp.float32), rope_upd.astype(jnp.float32))) * QDIM ** -0.5
        visible = jnp.arange(CTX)[None, None, :] <= positions[:, None, None]
        scores = jnp.where(visible, scores, -1e30)
        attn_prob = jax.nn.softmax(scores, axis=-1).astype(jnp.bfloat16)
        out_lat = jnp.einsum('chl,lk->chk', attn_prob.astype(jnp.float32), lat_f32).astype(jnp.bfloat16)
        out_head = jnp.einsum('chk,khv->chv', out_lat.astype(jnp.float32), w_uv.astype(jnp.float32)).astype(jnp.bfloat16)
        attn_out = jnp.dot(out_head.reshape(CHUNK, HEADS * VDIM), w_o.reshape(HEADS * VDIM, HID), preferred_element_type=jnp.float32).astype(jnp.bfloat16)
        hidden = (x_req.astype(jnp.float32) + attn_out.astype(jnp.float32)).astype(jnp.bfloat16)
        return hidden, lat_upd, rope_upd

    reqs_all = GROUP * REQS
    hidden, lat_upd, rope_upd = lax.map(one_request, (x.reshape(reqs_all, CHUNK, HID), chunk_len.reshape(reqs_all), ctx_len.reshape(reqs_all), lat_cache.reshape(reqs_all, CTX, RANK), rope_cache.reshape(reqs_all, CTX, ROPE)))
    rows = GROUP * TOKENS
    pairs = rows * TOP
    flat_h = hidden.reshape(rows, HID)
    normed = rms_norm(flat_h, g_ffn)
    valid = (jnp.arange(CHUNK)[None, :] < chunk_len.reshape(reqs_all, 1)).reshape(rows)
    route_prob = jax.nn.softmax(jnp.dot(normed, w_router, preferred_element_type=jnp.float32), axis=-1)
    choice = topk_idx.reshape(rows, TOP)
    gates = jnp.take_along_axis(route_prob, choice, axis=1)
    shared_act = (jax.nn.silu(jnp.dot(normed, w_sh_gate, preferred_element_type=jnp.float32)) * jnp.dot(normed, w_sh_up, preferred_element_type=jnp.float32)).astype(jnp.bfloat16)
    shared_out = jnp.dot(shared_act, w_sh_down, preferred_element_type=jnp.float32)
    pair_ok = jnp.repeat(valid, TOP)
    pair_key = jnp.where(pair_ok, choice.reshape(pairs), EXPERTS)
    counts = jnp.bincount(pair_key, length=EXPERTS + 1)
    padded = (counts[:EXPERTS] + BLOCK_ROWS - 1) // BLOCK_ROWS * BLOCK_ROWS
    pad_start = jnp.cumsum(padded) - padded
    raw_start = jnp.cumsum(counts) - counts
    order = jnp.argsort(pair_key, stable=True)
    sorted_key = pair_key[order]
    num_blocks = pairs // BLOCK_ROWS + EXPERTS + 1
    slots = num_blocks * BLOCK_ROWS
    start_ext = jnp.concatenate([pad_start, jnp.full((1,), slots, pad_start.dtype)])
    slot_of_sorted = start_ext[sorted_key] + jnp.arange(pairs) - raw_start[sorted_key]
    slot_pair = jnp.full((slots,), pairs, order.dtype).at[slot_of_sorted].set(order, mode='drop')
    slot_token = slot_pair // TOP
    gate_ext = jnp.concatenate([gates.reshape(pairs), jnp.zeros((1,), jnp.float32)])
    slot_gate = gate_ext[slot_pair]
    block_start = jnp.arange(num_blocks) * BLOCK_ROWS
    block_exp = jnp.clip(jnp.sum(pad_start[None, :] <= block_start[:, None], axis=1) - 1, 0, EXPERTS - 1)
    normed_ext = jnp.concatenate([normed, jnp.zeros((1, HID), jnp.bfloat16)])

    def expert_block(routed, args):
        tok_ids, tok_gate, exp_id = args
        block_in = normed_ext[tok_ids].astype(jnp.float32)
        gate_w = lax.dynamic_index_in_dim(w_exp_gate, exp_id, 0, keepdims=False).astype(jnp.float32)
        up_w = lax.dynamic_index_in_dim(w_exp_up, exp_id, 0, keepdims=False).astype(jnp.float32)
        down_w = lax.dynamic_index_in_dim(w_exp_down, exp_id, 0, keepdims=False).astype(jnp.float32)
        act = (jax.nn.silu(jnp.dot(block_in, gate_w)) * jnp.dot(block_in, up_w)).astype(jnp.bfloat16)
        block_out = jnp.dot(act.astype(jnp.float32), down_w).astype(jnp.bfloat16)
        routed = routed.at[tok_ids].add(tok_gate[:, None] * block_out.astype(jnp.float32), mode='drop')
        return routed, tok_ids[0]

    routed = lax.scan(expert_block, jnp.zeros((rows, HID), jnp.float32), (slot_token.reshape(num_blocks, BLOCK_ROWS), slot_gate.reshape(num_blocks, BLOCK_ROWS), block_exp))[0]
    total = flat_h.astype(jnp.float32) + shared_out + routed
    result = jnp.where(valid[:, None], total, 0.0).astype(jnp.bfloat16).reshape(GROUP, REQS, CHUNK, HID)
    return result, lat_upd.reshape(GROUP, REQS, CTX, RANK), rope_upd.reshape(GROUP, REQS, CTX, ROPE)
```

```python
import functools

import jax
import jax.numpy as jnp
from jax import lax
from jax.experimental import pallas as pl
from jax.experimental.pallas import tpu as pltpu
from jax.sharding import PartitionSpec as P

EPS = 1e-6
THETA = 10000.0


def rms_norm(vals, gain):
    vals_f32 = vals.astype(jnp.float32)
    inv_rms = lax.rsqrt(jnp.mean(vals_f32 * vals_f32, axis=-1, keepdims=True) + EPS)
    return (vals_f32 * inv_rms * gain.astype(jnp.float32)).astype(jnp.bfloat16)


def rope_tables(positions, half):
    inv_freq = THETA ** (-2.0 * jnp.arange(half, dtype=jnp.float32) / (2 * half))
    angle = positions.astype(jnp.float32)[..., None] * inv_freq
    return jnp.cos(angle), jnp.sin(angle)


def rotate(vals, cos_tab, sin_tab):
    half = cos_tab.shape[-1]
    first = vals[..., :half]
    second = vals[..., half:]
    return jnp.concatenate([first * cos_tab - second * sin_tab, second * cos_tab + first * sin_tab], axis=-1)


def write_window(cache_row, new_rows, start, keep):
    old_rows = lax.dynamic_slice_in_dim(cache_row, start, new_rows.shape[0], axis=0)
    merged = jnp.where(keep[:, None], new_rows, old_rows)
    return lax.dynamic_update_slice_in_dim(cache_row, merged, start, axis=0)


def attention_block(x_in, chunk_len, ctx_len, lat_cache, rope_cache, g_attn, w_q, w_dkv, g_kv, w_kr, w_uk, w_uv, w_o):
    chunk = x_in.shape[2]
    ctx_max = lat_cache.shape[2]
    rope_dim = w_kr.shape[1]
    nope_dim = w_q.shape[2] - rope_dim
    scale = w_q.shape[2] ** -0.5
    normed = rms_norm(x_in, g_attn)
    q_full = jnp.einsum('brcd,dhq->brchq', normed, w_q, preferred_element_type=jnp.float32).astype(jnp.bfloat16)
    positions = ctx_len[:, :, None] + jnp.arange(chunk)
    cos_tab, sin_tab = rope_tables(positions, rope_dim // 2)
    q_rope = rotate(q_full[..., nope_dim:].astype(jnp.float32), cos_tab[..., None, :], sin_tab[..., None, :]).astype(jnp.bfloat16)
    q_lat = jnp.einsum('brchn,khn->brchk', q_full[..., :nope_dim], w_uk, preferred_element_type=jnp.float32).astype(jnp.bfloat16)
    lat_new = rms_norm(jnp.einsum('brcd,dk->brck', normed, w_dkv, preferred_element_type=jnp.float32), g_kv)
    rope_new = rotate(jnp.einsum('brcd,dp->brcp', normed, w_kr, preferred_element_type=jnp.float32), cos_tab, sin_tab).astype(jnp.bfloat16)
    keep = jnp.arange(chunk) < chunk_len[:, :, None]
    writer = jax.vmap(jax.vmap(write_window))
    lat_upd = writer(lat_cache, lat_new, ctx_len, keep)
    rope_upd = writer(rope_cache, rope_new, ctx_len, keep)
    key_pos = jnp.arange(ctx_max)

    def one_request(index):
        q_lat_req = lax.dynamic_index_in_dim(q_lat, index, axis=1, keepdims=False)
        q_rope_req = lax.dynamic_index_in_dim(q_rope, index, axis=1, keepdims=False)
        lat_req = lax.dynamic_index_in_dim(lat_upd, index, axis=1, keepdims=False)
        rope_req = lax.dynamic_index_in_dim(rope_upd, index, axis=1, keepdims=False)
        pos_req = lax.dynamic_index_in_dim(positions, index, axis=1, keepdims=False)
        scores = (jnp.einsum('bchk,blk->bchl', q_lat_req, lat_req, preferred_element_type=jnp.float32) + jnp.einsum('bchp,blp->bchl', q_rope_req, rope_req, preferred_element_type=jnp.float32)) * scale
        visible = key_pos[None, None, None, :] <= pos_req[:, :, None, None]
        scores = jnp.where(visible, scores, -1e30)
        attn_prob = jax.nn.softmax(scores, axis=-1).astype(jnp.bfloat16)
        return jnp.einsum('bchl,blk->bchk', attn_prob, lat_req, preferred_element_type=jnp.float32).astype(jnp.bfloat16)

    out_lat = lax.map(one_request, jnp.arange(x_in.shape[1]))
    out_head = jnp.einsum('rbchk,khv->brchv', out_lat, w_uv, preferred_element_type=jnp.float32).astype(jnp.bfloat16)
    attn_out = jnp.einsum('brchv,hvd->brcd', out_head, w_o, preferred_element_type=jnp.float32).astype(jnp.bfloat16)
    hidden = (x_in.astype(jnp.float32) + attn_out.astype(jnp.float32)).astype(jnp.bfloat16)
    return hidden, lat_upd, rope_upd


MESH_ID = pl.DeviceIdType.MESH
F32 = jnp.float32
BF16 = jnp.bfloat16
LANES = 128
SUB = 8


def moe_kernel(dims, u_ref, h_ref, tk_ref, len_ref, wr_ref, wsg, wsu, wsd, wg, wu, wd, y_ref, rows_all, back, tk_all, slot_in, slot_out, gates, sh_act, picked, act, sent, row_exp, acc, w_gu, w_dn, stage, three, tk_s, tk_r, ring_s, ring_r, sib_s, sib_r, own_s, own_r, back_s, back_r, gu_sem, dn_sem, st_sem, th_sem, loc_sem):
    group, tokens, width, cap, local, ff, shared_ff, top_k, experts = dims
    ring = group // 2
    half = tokens // 2
    chunk_rows = 4 * cap
    gu_tiles = local * ff // LANES
    per_exp = ff // LANES
    sh_tiles = shared_ff // LANES
    dn_cols = w_dn.shape[2]
    dn_tiles = width // dn_cols
    me = lax.axis_index('dpa')
    zpos = lax.div(me, 2)
    core = lax.rem(me, 2)

    def dev(zz, cc):
        return lax.rem(zz + 2 * ring, ring) * 2 + cc

    def remote(src, dst, s_sem, r_sem, to):
        return pltpu.make_async_remote_copy(src_ref=src, dst_ref=dst, send_sem=s_sem, recv_sem=r_sem, device_id={'dpa': to}, device_id_type=MESH_ID)

    barrier = pltpu.get_barrier_semaphore()

    def greet(i, carry):
        pl.semaphore_signal(barrier, inc=1, device_id={'dpa': lax.rem(me + i, group)}, device_id_type=MESH_ID)
        return carry

    lax.fori_loop(1, group, greet, 0)
    pl.semaphore_wait(barrier, group - 1)

    def tk_copy(i, owner):
        return remote(tk_ref, tk_all.at[owner], tk_s.at[i], tk_r.at[i], lax.rem(me + i, group))

    def tk_start(i, carry):
        tk_copy(i, me).start()
        return carry

    lax.fori_loop(1, group, tk_start, 0)

    def ring_copy(way, hop, part, sending):
        sign = 1 - 2 * way
        owner = dev(zpos - sign * (hop - 1 if sending else hop), core)
        rows = pl.ds(part * half, half)
        dst = rows_all.at[owner, rows]
        src = u_ref.at[rows] if sending and hop == 1 else dst
        return remote(src, dst, ring_s.at[way, hop - 1, part], ring_r.at[way, hop - 1, part], dev(zpos + sign, core))

    def sib_copy(way, hop, part, cc):
        sign = 1 - 2 * way
        block = rows_all.at[dev(zpos - sign * hop, cc), pl.ds(part * half, half)]
        return remote(block, block, sib_s.at[way, hop - 1, part], sib_r.at[way, hop - 1, part], dev(zpos, 1 - core))

    far = ring // 2

    def in_ring(way, hop, part):
        return hop < far or (hop == far and part == way)

    def own_copy(cc):
        return remote(u_ref, rows_all.at[dev(zpos, cc)], own_s, own_r, dev(zpos, 1 - core))

    keep_own = pltpu.make_async_copy(u_ref, rows_all.at[me], loc_sem.at[0])
    for part in range(2):
        for way in range(2):
            ring_copy(way, 1, part, True).start()
    own_copy(core).start()
    keep_own.start()

    def relay(hop, part):
        for way in range(2):
            if in_ring(way, hop, part):
                ring_copy(way, hop, part, False).wait_recv()
                if in_ring(way, hop + 1, part):
                    ring_copy(way, hop + 1, part, True).start()
                sib_copy(way, hop, part, core).start()

    def gu_copies(shared, t):
        slot = lax.rem(t, w_gu.shape[0])
        if shared:
            cols = pl.ds(pl.multiple_of(t * LANES, LANES), LANES)
            srcs = (wsg.at[:, cols], wsu.at[:, cols])
        else:
            cols = pl.ds(pl.multiple_of(lax.rem(t, per_exp) * LANES, LANES), LANES)
            exp = lax.div(t, per_exp)
            srcs = (wg.at[exp, :, cols], wu.at[exp, :, cols])
        return [pltpu.make_async_copy(src, w_gu.at[slot, :, pl.ds(i * LANES, LANES)], gu_sem.at[slot, i]) for i, src in enumerate(srcs)]

    def dn_copy(shared, t):
        slot = lax.rem(t, w_dn.shape[0])
        cols = pl.ds(pl.multiple_of(t * dn_cols, dn_cols), dn_cols)
        if shared:
            return pltpu.make_async_copy(wsd.at[:, cols], w_dn.at[slot, pl.ds(0, shared_ff)], dn_sem.at[slot])
        return pltpu.make_async_copy(wd.at[:, cols], w_dn.at[slot], dn_sem.at[slot])

    gu_ahead = w_gu.shape[0] - 1
    dn_ahead = w_dn.shape[0] - 1

    def gu_start(shared, t):
        for copy in gu_copies(shared, t):
            copy.start()

    def prime_gu(shared):
        for t in range(gu_ahead):
            gu_start(shared, jnp.int32(t))

    def prime_dn(shared):
        for t in range(dn_ahead):
            dn_copy(shared, jnp.int32(t)).start()

    prime_gu(True)
    prime_dn(True)

    logits = lax.dot_general(wr_ref[...], u_ref[...], (((1,), (1,)), ((), ())), preferred_element_type=F32)
    shifted = jnp.exp(logits - jnp.max(logits, axis=0, keepdims=True))
    prob = shifted / jnp.sum(shifted, axis=0, keepdims=True)
    exp_row = lax.broadcasted_iota(jnp.int32, (experts, tokens), 0)
    for k in range(SUB):
        if k < top_k:
            gates[k:k + 1, :] = jnp.sum(jnp.where(exp_row == tk_ref[k:k + 1, :], prob, 0.0), axis=0, keepdims=True)
        else:
            gates[k:k + 1, :] = jnp.zeros((1, tokens), F32)

    def glu(both):
        gate = both[:, :LANES]
        return gate * jax.nn.sigmoid(gate) * both[:, LANES:]

    def sh_gu(t, carry):
        @pl.when(t + gu_ahead < sh_tiles)
        def _():
            gu_start(True, t + gu_ahead)

        for copy in gu_copies(True, t):
            copy.wait()
        both = jnp.dot(u_ref[...], w_gu[lax.rem(t, w_gu.shape[0])], preferred_element_type=F32)
        sh_act[:, pl.ds(pl.multiple_of(t * LANES, LANES), LANES)] = glu(both).astype(BF16)
        return carry

    lax.fori_loop(0, sh_tiles, sh_gu, 0)
    prime_gu(False)
    relay(1, 0)

    def sh_dn(t, carry):
        @pl.when(t + dn_ahead < dn_tiles)
        def _():
            dn_copy(True, t + dn_ahead).start()

        dn_copy(True, t).wait()
        cols = pl.ds(pl.multiple_of(t * dn_cols, dn_cols), dn_cols)
        tile = w_dn[lax.rem(t, w_dn.shape[0]), :shared_ff]
        acc[:, cols] = h_ref[:, cols].astype(F32) + jnp.dot(sh_act[...], tile, preferred_element_type=F32)
        return carry

    lax.fori_loop(0, dn_tiles, sh_dn, 0)
    prime_dn(False)

    tk_all[me] = tk_ref[...]

    def tk_wait(i, carry):
        tk_copy(i, lax.rem(me - i + group, group)).wait_recv()
        return carry

    lax.fori_loop(1, group, tk_wait, 0)
    rows8 = group * SUB
    before = (lax.broadcasted_iota(jnp.int32, (tokens, tokens), 0) < lax.broadcasted_iota(jnp.int32, (tokens, tokens), 1)).astype(F32).astype(BF16)
    row_a = lax.broadcasted_iota(jnp.int32, (rows8, rows8), 0)
    row_b = lax.broadcasted_iota(jnp.int32, (rows8, rows8), 1)
    above = jnp.logical_and(row_b < row_a, lax.div(row_b, SUB) == lax.div(row_a, SUB)).astype(F32).astype(BF16)
    row_id = lax.broadcasted_iota(jnp.int32, (rows8, tokens), 0)
    is_choice = lax.rem(row_id, SUB) < top_k

    def slots(hit):
        ones = hit.astype(F32).astype(BF16)
        upto = jnp.dot(ones, before, preferred_element_type=F32)
        rows_up = jnp.sum(jnp.dot(above, ones, preferred_element_type=F32), axis=1, keepdims=True)
        return upto + rows_up

    all_tk = tk_all[...].reshape(rows8, tokens)
    hit_in = jnp.logical_and(is_choice, lax.div(all_tk, local) == me)
    own_len = jnp.broadcast_to(tk_all[:, top_k:top_k + 1, :], (group, SUB, tokens)).reshape(rows8, tokens)
    live = jnp.logical_and(hit_in, lax.broadcasted_iota(jnp.int32, (rows8, tokens), 1) < own_len)
    slot_in[...] = jnp.where(live, slots(hit_in), -1.0).reshape(group, SUB, tokens)
    own_tk = jnp.broadcast_to(tk_ref[...][None], (group, SUB, tokens)).reshape(rows8, tokens)
    hit_out = jnp.logical_and(is_choice, lax.div(own_tk, local) == lax.div(row_id, SUB))
    slot_out[...] = jnp.where(hit_out, slots(hit_out), -1.0).reshape(group, SUB, tokens)

    keep_own.wait()
    relay(1, 1)

    slot_row = lax.broadcasted_iota(jnp.int32, (cap, tokens), 0).astype(F32)

    def source(c, j):
        side = lax.div(j, 2)
        zz = zpos + (1 - side) * (c + 1) - side * lax.rem(c + 1, far)
        return dev(zz, lax.rem(j, 2))

    def send_back(c, j, to):
        block = sent.at[c, pl.ds(pl.multiple_of(j * cap, 16), cap)]
        return remote(block, back.at[me], back_s.at[c * 4 + j], back_r.at[c * 4 + lax.div(j, 2) * 2 + core], to)

    def chunk(c, carry):
        for hop in range(1, far + 1):
            @pl.when(c == hop - 1)
            def _():
                for part in range(2):
                    for way in range(2):
                        if in_ring(way, hop, part):
                            sib_copy(way, hop, part, 1 - core).wait_recv()
                if hop == far:
                    own_copy(1 - core).wait_recv()

        def load(j):
            slot = lax.rem(j, 2)
            return pltpu.make_async_copy(rows_all.at[source(c, j)], stage.at[slot], st_sem.at[slot])

        load(jnp.int32(0)).start()

        def gather(j, inner):
            @pl.when(j < 3)
            def _():
                load(j + 1).start()

            src = source(c, j)
            pick = jnp.zeros((cap, tokens), F32)
            which = jnp.zeros((cap, tokens), F32)
            for k in range(top_k):
                same = slot_row == slot_in[src, k:k + 1, :]
                pick = jnp.where(same, 1.0, pick)
                which = jnp.where(same, lax.rem(tk_all[src, k:k + 1, :], local).astype(F32), which)
            rows = pl.ds(pl.multiple_of(j * cap, 16), cap)
            row_exp[rows, :] = jnp.broadcast_to(jnp.sum(which, axis=1, keepdims=True), (cap, LANES))
            load(j).wait()
            picked[rows, :] = jnp.dot(pick.astype(BF16), stage[lax.rem(j, 2)], preferred_element_type=F32).astype(BF16)
            return inner

        lax.fori_loop(0, 4, gather, 0)

        @pl.when(c > 0)
        def _():
            for j in range(4):
                send_back(c - 1, j, source(c - 1, jnp.int32(j))).start()

        def gate_up(t, inner):
            @pl.when(t + gu_ahead < gu_tiles)
            def _():
                gu_start(False, t + gu_ahead)

            for copy in gu_copies(False, t):
                copy.wait()
            for when_c, when_t, hop, part in EVENTS:
                @pl.when(jnp.logical_and(c == when_c, t == when_t * gu_tiles // 44))
                def _():
                    relay(hop, part)

            both = jnp.dot(picked[...], w_gu[lax.rem(t, w_gu.shape[0])], preferred_element_type=F32)
            mine = row_exp[...] == lax.div(t, per_exp).astype(F32)
            act[:, pl.ds(pl.multiple_of(t * LANES, LANES), LANES)] = jnp.where(mine, glu(both), 0.0).astype(BF16)
            return inner

        lax.fori_loop(0, gu_tiles, gate_up, 0)

        @pl.when(c < 3)
        def _():
            prime_gu(False)

        def down(t, inner):
            @pl.when(t + dn_ahead < dn_tiles)
            def _():
                dn_copy(False, t + dn_ahead).start()

            dn_copy(False, t).wait()
            out = jnp.dot(act[...], w_dn[lax.rem(t, w_dn.shape[0])], preferred_element_type=F32)
            sent[c, :, pl.ds(pl.multiple_of(t * dn_cols, dn_cols), dn_cols)] = out.astype(BF16)
            return inner

        lax.fori_loop(0, dn_tiles, down, 0)

        @pl.when(c < 3)
        def _():
            prime_dn(False)

        return carry

    lax.fori_loop(0, 4, chunk, 0)
    for j in range(2):
        send_back(jnp.int32(3), jnp.int32(j), source(jnp.int32(3), jnp.int32(j))).start()
    send_back(jnp.int32(3), 3 - core, dev(zpos, 1 - core)).start()
    mine = pltpu.make_async_copy(sent.at[3, pl.ds(pl.multiple_of((2 + core) * cap, 16), cap)], back.at[me], back_r.at[14 + core])
    mine.start()

    def combine(i, carry):
        at = i + lax.div(i, 12) * (lax.rem(i + 2, 4) - lax.rem(i, 4))
        c = lax.div(at, 4)
        side = lax.rem(lax.div(at, 2), 2)
        zz = zpos - (1 - side) * (c + 1) + side * lax.rem(c + 1, far)
        who = dev(zz, lax.rem(at, 2))
        remote(sent.at[0, pl.ds(0, cap)], back.at[who], back_s.at[0], back_r.at[at], dev(zpos, 1 - core)).wait_recv()
        loads = [pltpu.make_async_copy(back.at[who], three.at[pl.ds(r * cap, cap)], th_sem.at[r]) for r in range(3)]
        for copy in loads:
            copy.start()
        mix = jnp.zeros((cap, tokens), F32)
        for k in range(top_k):
            mix = jnp.where(slot_row == slot_out[who, k:k + 1, :], gates[k:k + 1, :], mix)
        high = mix.astype(BF16)
        rest = mix - high.astype(F32)
        mid = rest.astype(BF16)
        low = (rest - mid.astype(F32)).astype(BF16)
        parts = jnp.concatenate([high, mid, low], axis=0)
        for copy in loads:
            copy.wait()

        def add(t, inner):
            cols = pl.ds(pl.multiple_of(t * 512, 512), 512)
            acc[:, cols] += lax.dot_general(parts, three[:, cols], (((0,), (0,)), ((), ())), preferred_element_type=F32)
            return inner

        lax.fori_loop(0, width // 512, add, 0)
        return carry

    lax.fori_loop(0, group, combine, 0)
    row = lax.broadcasted_iota(jnp.int32, (tokens, width), 0)
    y_ref[...] = jnp.where(row < len_ref[0], acc[...], 0.0).astype(BF16)

    for i in range(1, group):
        tk_copy(i, me).wait_send()
    for way in range(2):
        for hop in range(1, far + 1):
            for part in range(2):
                if in_ring(way, hop, part):
                    ring_copy(way, hop, part, True).wait_send()
                    sib_copy(way, hop, part, core).wait_send()
    own_copy(core).wait_send()
    for c in range(3):
        for j in range(4):
            send_back(jnp.int32(c), jnp.int32(j), source(jnp.int32(c), jnp.int32(j))).wait_send()
    for j in range(2):
        send_back(jnp.int32(3), jnp.int32(j), source(jnp.int32(3), jnp.int32(j))).wait_send()
    send_back(jnp.int32(3), 3 - core, dev(zpos, 1 - core)).wait_send()


EVENTS = ((0, 16, 2, 0), (0, 40, 2, 1), (1, 4, 3, 0), (1, 24, 3, 1), (1, 43, 4, 0), (1, 43, 4, 1))


def moe_layer(group, u, h, topk, chunk_len, w_router, wsg, wsu, wsd, wg, wu, wd):
    tokens, width = u.shape
    top_k = topk.shape[1]
    local, _, ff = wg.shape
    shared_ff = wsg.shape[1]
    experts = w_router.shape[1]
    cap = tokens * top_k // group
    length = jnp.broadcast_to(chunk_len.reshape(1, 1), (SUB - top_k, tokens))
    tk = jnp.concatenate([topk.T, length], axis=0)
    dims = (group, tokens, width, cap, local, ff, shared_ff, top_k, experts)
    far = group // 4
    vmem = pl.BlockSpec(memory_space=pltpu.VMEM)
    hbm = pl.BlockSpec(memory_space=pl.ANY)
    smem = pl.BlockSpec(memory_space=pltpu.SMEM)
    dma = pltpu.SemaphoreType.DMA
    scratch = [
        pltpu.VMEM((group, SUB, tokens), jnp.int32),
        pltpu.VMEM((group, SUB, tokens), F32),
        pltpu.VMEM((group, SUB, tokens), F32),
        pltpu.VMEM((SUB, tokens), F32),
        pltpu.VMEM((tokens, shared_ff), BF16),
        pltpu.VMEM((4 * cap, width), BF16),
        pltpu.VMEM((4 * cap, local * ff), BF16),
        pltpu.VMEM((4, 4 * cap, width), BF16),
        pltpu.VMEM((4 * cap, LANES), F32),
        pltpu.VMEM((tokens, width), F32),
        pltpu.VMEM((4, width, 2 * LANES), BF16),
        pltpu.VMEM((3, local * ff, 256), BF16),
        pltpu.VMEM((2, tokens, width), BF16),
        pltpu.VMEM((3 * cap, width), BF16),
        dma((group,)), dma((group,)),
        dma((2, far, 2)), dma((2, far, 2)),
        dma((2, far, 2)), dma((2, far, 2)),
        dma, dma,
        dma((group,)), dma((group,)),
        dma((4, 2)), dma((3,)), dma((2,)), dma((3,)), dma((1,)),
    ]
    return pl.pallas_call(
        functools.partial(moe_kernel, dims),
        out_shape=[jax.ShapeDtypeStruct((tokens, width), BF16), jax.ShapeDtypeStruct((group, tokens, width), BF16), jax.ShapeDtypeStruct((group, cap, width), BF16)],
        in_specs=[vmem, vmem, vmem, smem, vmem] + [hbm] * 6,
        out_specs=[vmem, hbm, hbm],
        scratch_shapes=scratch,
        compiler_params=pltpu.CompilerParams(collective_id=0, has_side_effects=True, vmem_limit_bytes=67043328),
    )(u, h, tk, chunk_len.reshape(1), w_router.T, wsg, wsu, wsd, wg, wu, wd.reshape(local * ff, width))[0]


def solution(mesh):
    group = mesh.shape['dpa']
    tok_spec = P(('dp', 'dpa'))
    whole = P()
    exp_spec = P('dpa')

    def device_step(x_in, chunk_len, ctx_len, lat_cache, rope_cache, topk_idx, g_attn, w_q, w_dkv, g_kv, w_kr, w_uk, w_uv, w_o, g_ffn, w_router, w_sh_gate, w_sh_up, w_sh_down, w_exp_gate, w_exp_up, w_exp_down):
        hidden, lat_upd, rope_upd = attention_block(x_in, chunk_len, ctx_len, lat_cache, rope_cache, g_attn, w_q, w_dkv, g_kv, w_kr, w_uk, w_uv, w_o)
        chunk, width = hidden.shape[2:]
        flat_h = hidden.reshape(chunk, width)
        normed = rms_norm(flat_h, g_ffn)
        result = moe_layer(group, normed, flat_h, topk_idx.reshape(chunk, topk_idx.shape[-1]), chunk_len, w_router, w_sh_gate, w_sh_up, w_sh_down, w_exp_gate, w_exp_up, w_exp_down)
        return result.reshape(hidden.shape), lat_upd, rope_upd

    return jax.shard_map(device_step, mesh=mesh, in_specs=(tok_spec,) * 6 + (whole,) * 13 + (exp_spec,) * 3, out_specs=(tok_spec, tok_spec, tok_spec), check_vma=False)
```

```python
import functools

import jax
import jax.numpy as jnp
from jax import lax
from jax.experimental import pallas as pl
from jax.experimental.pallas import tpu as pltpu
from jax.sharding import PartitionSpec as P

EPS = 1e-6
THETA = 10000.0
MESH_ID = pl.DeviceIdType.MESH
F32 = jnp.float32
BF16 = jnp.bfloat16
LANES = 128
SUB = 8


def rms_norm(vals, gain):
    vals_f32 = vals.astype(jnp.float32)
    inv_rms = lax.rsqrt(jnp.mean(vals_f32 * vals_f32, axis=-1, keepdims=True) + EPS)
    return (vals_f32 * inv_rms * gain.astype(jnp.float32)).astype(jnp.bfloat16)


def rope_tables(positions, half):
    inv_freq = THETA ** (-2.0 * jnp.arange(half, dtype=jnp.float32) / (2 * half))
    angle = positions.astype(jnp.float32)[..., None] * inv_freq
    return jnp.cos(angle), jnp.sin(angle)


def attn_kernel(scale, len_ref, ctx_ref, x_hbm, gains_ref, tab_ref, dkv_hbm, kr_hbm, q_hbm, lat_hbm, rope_hbm, uk_hbm, uv_hbm, wo_hbm, h_ref, u_ref, lat_ref, rope_ref, x, dkv, kr, q, lat_old, rope_old, uk, uv, wo, uk_wide, uv_wide, turned, lat_t, rope_rows, heads_out, sems, q_sems):
    heads, qdim, width = q.shape
    ctx_max, rank = lat_old.shape
    rope_dim = rope_old.shape[0]
    nope = qdim - rope_dim
    half = rope_dim // 2
    chunk = x.shape[0]
    copies = [pltpu.make_async_copy(src, dst, sems.at[i]) for i, (src, dst) in enumerate(((x_hbm, x), (dkv_hbm, dkv), (kr_hbm, kr), (lat_hbm, lat_old), (rope_hbm, rope_old), (uk_hbm, uk), (uv_hbm, uv), (wo_hbm, wo)))]

    def q_copy(i):
        both = pl.ds(2 * i, 2)
        return pltpu.make_async_copy(q_hbm.at[both], q.at[both], q_sems.at[i])

    for copy in copies[:5]:
        copy.start()
    for i in range(2):
        q_copy(i).start()
    for copy in copies[5:7]:
        copy.start()
    for i in range(2, heads // 2):
        q_copy(i).start()
    copies[7].start()
    clen = len_ref[0]
    ctx = ctx_ref[0]
    cos_tab = tab_ref[:half, :]
    sin_tab = tab_ref[half:, :]

    def roped(vals):
        first = vals[:half]
        second = vals[half:]
        return jnp.concatenate([first * cos_tab - second * sin_tab, second * cos_tab + first * sin_tab], axis=0).astype(BF16)

    def normed(vals, gain):
        return vals * lax.rsqrt(jnp.mean(vals * vals, axis=1, keepdims=True) + EPS) * gain

    copies[0].wait()
    a = normed(x[...].astype(F32), gains_ref[:, :width]).astype(BF16)
    turned[...] = jnp.transpose(a.astype(F32)).astype(BF16)
    copies[1].wait()
    lat_new = normed(jnp.dot(a, dkv[...], preferred_element_type=F32), gains_ref[:, 2 * width:]).astype(BF16)
    copies[2].wait()
    rope_new = roped(jnp.dot(kr[...], turned[...], preferred_element_type=F32))
    place = lax.broadcasted_iota(jnp.int32, (ctx_max, chunk), 0) - ctx
    row = lax.broadcasted_iota(jnp.int32, (ctx_max, chunk), 1)
    move = jnp.where(jnp.logical_and(place == row, row < clen), 1.0, 0.0).astype(BF16)
    pos = lax.broadcasted_iota(jnp.int32, (ctx_max, rank), 0) - ctx
    copies[3].wait()
    lat = jnp.where(jnp.logical_and(pos >= 0, pos < clen), jnp.dot(move, lat_new, preferred_element_type=F32), lat_old[...].astype(F32))
    lat_ref[...] = lat.astype(BF16)
    lat_t[...] = jnp.transpose(lat).astype(BF16)
    place = lax.broadcasted_iota(jnp.int32, (chunk, ctx_max), 1) - ctx
    row = lax.broadcasted_iota(jnp.int32, (chunk, ctx_max), 0)
    move = jnp.where(jnp.logical_and(place == row, row < clen), 1.0, 0.0).astype(BF16)
    pos = lax.broadcasted_iota(jnp.int32, (rope_dim, ctx_max), 1) - ctx
    copies[4].wait()
    rope = jnp.where(jnp.logical_and(pos >= 0, pos < clen), jnp.dot(rope_new, move, preferred_element_type=F32), rope_old[...].astype(F32))
    rope_ref[...] = rope.astype(BF16)
    rope_rows[...] = jnp.transpose(jnp.concatenate([rope, jnp.zeros_like(rope)], axis=0)).astype(BF16)
    copies[5].wait()
    uk_wide[...] = uk[...].astype(F32)
    copies[6].wait()
    uv_wide[...] = uv[...].astype(F32)
    seen = lax.broadcasted_iota(jnp.int32, (ctx_max, chunk), 0) - lax.broadcasted_iota(jnp.int32, (ctx_max, chunk), 1) <= ctx
    factor = scale * 1.4426950408889634

    def pair(i, carry):
        q_copy(i).wait()
        both = jnp.dot(q[pl.ds(2 * i, 2)].reshape(2 * qdim, width), turned[...], preferred_element_type=F32).astype(BF16)
        lats = []
        ropes = []
        for k in range(2):
            mine = both[k * qdim:(k + 1) * qdim]
            up = uk_wide[pl.ds(2 * i + k, rank, stride=heads), :].astype(BF16)
            lats.append(jnp.dot(up, mine[:nope], preferred_element_type=F32).astype(BF16))
            ropes.append(roped(mine[nope:].astype(F32)))
        ropes = jnp.concatenate(ropes, axis=1)
        scores = jnp.dot(lat_ref[...], jnp.concatenate(lats, axis=1), preferred_element_type=F32) + jnp.dot(rope_rows[:, :rope_dim], ropes, preferred_element_type=F32)
        probs = []
        for k in range(2):
            mine = jnp.where(seen, scores[:, k * chunk:(k + 1) * chunk], -1e30)
            weight = jnp.exp2((mine - jnp.max(mine, axis=0, keepdims=True)) * factor)
            probs.append((weight * (1.0 / jnp.sum(weight, axis=0, keepdims=True))).astype(BF16))
        out = jnp.dot(lat_t[...], jnp.concatenate(probs, axis=1), preferred_element_type=F32).astype(BF16)
        for k in range(2):
            up = uv_wide[pl.ds(2 * i + k, rank, stride=heads), :].astype(BF16)
            mine = lax.dot_general(out[:, k * chunk:(k + 1) * chunk], up, (((0,), (0,)), ((), ())), preferred_element_type=F32)
            heads_out[:, pl.ds(pl.multiple_of((2 * i + k) * nope, nope), nope)] = mine.astype(BF16)
        return carry

    lax.fori_loop(0, heads // 2, pair, 0)
    copies[7].wait()

    def project(t, total):
        cols = pl.ds(pl.multiple_of(t * 256, 256), 256)
        out = jnp.dot(heads_out[...], wo[:, cols], preferred_element_type=F32).astype(BF16)
        hidden = (x[:, cols].astype(F32) + out.astype(F32)).astype(BF16)
        h_ref[:, cols] = hidden
        wide_h = hidden.astype(F32)
        return total + jnp.sum(wide_h * wide_h, axis=1, keepdims=True)

    total = lax.fori_loop(0, width // 256, project, jnp.zeros((chunk, 1), F32))
    inv = lax.rsqrt(total / width + EPS)
    u_ref[...] = (h_ref[...].astype(F32) * inv * gains_ref[:, width:2 * width]).astype(BF16)


def attention_block(x, chunk_len, ctx_len, lat_cache, rope_cache, g_attn, w_q, w_dkv, g_kv, w_kr, w_uk, w_uv, w_o, g_ffn):
    chunk, width = x.shape
    ctx_max, rank = lat_cache.shape
    rope_dim = rope_cache.shape[1]
    heads, qdim = w_q.shape[1:]
    nope = qdim - rope_dim
    vdim = w_uv.shape[2]
    tab = jnp.concatenate(rope_tables(ctx_len.reshape(1) + jnp.arange(chunk), rope_dim // 2), axis=1).T
    gains = jnp.concatenate([g_attn, g_ffn, g_kv]).astype(F32).reshape(1, 2 * width + rank)
    vmem = pl.BlockSpec(memory_space=pltpu.VMEM)
    hbm = pl.BlockSpec(memory_space=pl.ANY)
    smem = pl.BlockSpec(memory_space=pltpu.SMEM)
    low = [(chunk, width), (width, rank), (rope_dim, width), (heads, qdim, width), (ctx_max, rank), (rope_dim, ctx_max), (rank * heads, nope), (rank * heads, vdim), (heads * vdim, width)]
    wide = [(rank * heads, nope), (rank * heads, vdim)]
    more = [(width, chunk), (rank, ctx_max), (ctx_max, 2 * rope_dim), (chunk, heads * vdim)]
    hidden, normed, lat, rope = pl.pallas_call(
        functools.partial(attn_kernel, qdim ** -0.5),
        out_shape=[jax.ShapeDtypeStruct((chunk, width), BF16), jax.ShapeDtypeStruct((chunk, width), BF16), jax.ShapeDtypeStruct((ctx_max, rank), BF16), jax.ShapeDtypeStruct((rope_dim, ctx_max), BF16)],
        in_specs=[smem, smem, hbm, vmem, vmem] + [hbm] * 8,
        out_specs=[vmem] * 4,
        scratch_shapes=[pltpu.VMEM(shape, BF16) for shape in low] + [pltpu.VMEM(shape, F32) for shape in wide] + [pltpu.VMEM(shape, BF16) for shape in more] + [pltpu.SemaphoreType.DMA((8,)), pltpu.SemaphoreType.DMA((heads // 2,))],
        compiler_params=pltpu.CompilerParams(vmem_limit_bytes=67043328),
    )(chunk_len.reshape(1), ctx_len.reshape(1), x, gains, tab, w_dkv, w_kr.T, w_q.transpose(1, 2, 0), lat_cache, rope_cache.T, w_uk.reshape(rank * heads, nope), w_uv.reshape(rank * heads, vdim), w_o.reshape(heads * vdim, width))
    return hidden, normed, lat, rope.T


def moe_kernel(dims, u_ref, h_ref, tk_ref, len_ref, wr_ref, wsg, wsu, wsd, wg, wu, wd, y_ref, rows_all, tk_all, slot_in, slot_out, gates, sh_act, picked, act, sent, row_exp, acc, w_gu, w_dn, stage, three, back, halfway, tk_s, tk_r, ring_s, ring_r, sib_s, sib_r, own_s, own_r, back_s, back_r, leg_s, leg_r, fwd_s, gu_sem, dn_sem, st_sem, loc_sem):
    group, tokens, width, cap, local, ff, shared_ff, top_k, experts = dims
    ring = group // 2
    half = tokens // 2
    chunk_rows = 4 * cap
    gu_tiles = local * ff // (2 * LANES)
    per_exp = ff // LANES
    sh_tiles = shared_ff // (2 * LANES)
    dn_cols = w_dn.shape[2]
    dn_tiles = width // dn_cols
    me = lax.axis_index('dpa')
    zpos = lax.div(me, 2)
    core = lax.rem(me, 2)

    def dev(zz, cc):
        return lax.rem(zz + 2 * ring, ring) * 2 + cc

    def remote(src, dst, s_sem, r_sem, to):
        return pltpu.make_async_remote_copy(src_ref=src, dst_ref=dst, send_sem=s_sem, recv_sem=r_sem, device_id={'dpa': to}, device_id_type=MESH_ID)

    barrier = pltpu.get_barrier_semaphore()

    def greet(i, carry):
        pl.semaphore_signal(barrier, inc=1, device_id={'dpa': lax.rem(me + i, group)}, device_id_type=MESH_ID)
        return carry

    lax.fori_loop(1, group, greet, 0)
    pl.semaphore_wait(barrier, group - 1)

    def tk_copy(i, owner):
        return remote(tk_ref, tk_all.at[owner], tk_s.at[i], tk_r.at[i], lax.rem(me + i, group))

    def tk_start(i, carry):
        tk_copy(i, me).start()
        return carry

    lax.fori_loop(1, group, tk_start, 0)

    def ring_copy(way, hop, part, sending):
        sign = 1 - 2 * way
        owner = dev(zpos - sign * (hop - 1 if sending else hop), core)
        rows = pl.ds(part * half, half)
        dst = rows_all.at[owner, rows]
        src = u_ref.at[rows] if sending and hop == 1 else dst
        return remote(src, dst, ring_s.at[way, hop - 1, part], ring_r.at[way, hop - 1, part], dev(zpos + sign, core))

    def sib_copy(way, hop, part, cc):
        sign = 1 - 2 * way
        block = rows_all.at[dev(zpos - sign * hop, cc), pl.ds(part * half, half)]
        return remote(block, block, sib_s.at[way, hop - 1, part], sib_r.at[way, hop - 1, part], dev(zpos, 1 - core))

    far = ring // 2

    def in_ring(way, hop, part):
        return hop < far or (hop == far and part == way)

    def own_copy(cc):
        return remote(u_ref, rows_all.at[dev(zpos, cc)], own_s, own_r, dev(zpos, 1 - core))

    keep_own = pltpu.make_async_copy(u_ref, rows_all.at[me], loc_sem.at[0])
    for part in range(2):
        for way in range(2):
            ring_copy(way, 1, part, True).start()
    own_copy(core).start()
    keep_own.start()

    def relay(hop, part):
        for way in range(2):
            if in_ring(way, hop, part):
                ring_copy(way, hop, part, False).wait_recv()
                if in_ring(way, hop + 1, part):
                    ring_copy(way, hop + 1, part, True).start()
                sib_copy(way, hop, part, core).start()

    def gu_copies(shared, t):
        slot = lax.rem(t, w_gu.shape[0])
        if shared:
            cols = pl.ds(pl.multiple_of(t * 2 * LANES, 2 * LANES), 2 * LANES)
            srcs = (wsg.at[:, cols], wsu.at[:, cols])
        else:
            srcs = []
            for ref in (wg, wu):
                for part in range(2):
                    tile = 2 * t + part
                    cols = pl.ds(pl.multiple_of(lax.rem(tile, per_exp) * LANES, LANES), LANES)
                    srcs.append(ref.at[lax.div(tile, per_exp), :, cols])
        span = 4 * LANES // len(srcs)
        return [pltpu.make_async_copy(src, w_gu.at[slot, :, pl.ds(i * span, span)], gu_sem.at[slot, i]) for i, src in enumerate(srcs)]

    def dn_copy(shared, t):
        slot = lax.rem(t, w_dn.shape[0])
        cols = pl.ds(pl.multiple_of(t * dn_cols, dn_cols), dn_cols)
        if shared:
            return pltpu.make_async_copy(wsd.at[:, cols], w_dn.at[slot, pl.ds(0, shared_ff)], dn_sem.at[slot])
        return pltpu.make_async_copy(wd.at[:, cols], w_dn.at[slot], dn_sem.at[slot])

    gu_ahead = w_gu.shape[0] - 1
    dn_ahead = w_dn.shape[0] - 1

    def gu_start(shared, t):
        for copy in gu_copies(shared, t):
            copy.start()

    def prime_gu(shared):
        for t in range(gu_ahead):
            gu_start(shared, jnp.int32(t))

    def prime_dn(shared):
        for t in range(dn_ahead):
            dn_copy(shared, jnp.int32(t)).start()

    prime_gu(True)
    prime_dn(True)

    logits = lax.dot_general(wr_ref[...], u_ref[...], (((1,), (1,)), ((), ())), preferred_element_type=F32)
    shifted = jnp.exp(logits - jnp.max(logits, axis=0, keepdims=True))
    prob = shifted / jnp.sum(shifted, axis=0, keepdims=True)
    exp_row = lax.broadcasted_iota(jnp.int32, (experts, tokens), 0)
    for k in range(SUB):
        if k < top_k:
            gates[k:k + 1, :] = jnp.sum(jnp.where(exp_row == tk_ref[k:k + 1, :], prob, 0.0), axis=0, keepdims=True)
        else:
            gates[k:k + 1, :] = jnp.zeros((1, tokens), F32)

    def glu(both):
        gate = both[:, :2 * LANES]
        return gate * jax.nn.sigmoid(gate) * both[:, 2 * LANES:]

    def sh_gu(t, carry):
        @pl.when(t + gu_ahead < sh_tiles)
        def _():
            gu_start(True, t + gu_ahead)

        for copy in gu_copies(True, t):
            copy.wait()
        both = jnp.dot(u_ref[...], w_gu[lax.rem(t, w_gu.shape[0])], preferred_element_type=F32)
        sh_act[:, pl.ds(pl.multiple_of(t * 2 * LANES, 2 * LANES), 2 * LANES)] = glu(both).astype(BF16)
        return carry

    lax.fori_loop(0, sh_tiles, sh_gu, 0)
    prime_gu(False)
    relay(1, 0)

    def sh_dn(t, carry):
        @pl.when(t + dn_ahead < dn_tiles)
        def _():
            dn_copy(True, t + dn_ahead).start()

        dn_copy(True, t).wait()
        cols = pl.ds(pl.multiple_of(t * dn_cols, dn_cols), dn_cols)
        tile = w_dn[lax.rem(t, w_dn.shape[0]), :shared_ff]
        acc[:, cols] = h_ref[:, cols].astype(F32) + jnp.dot(sh_act[...], tile, preferred_element_type=F32)
        return carry

    lax.fori_loop(0, dn_tiles, sh_dn, 0)
    prime_dn(False)

    tk_all[me] = tk_ref[...]

    def tk_wait(i, carry):
        tk_copy(i, lax.rem(me - i + group, group)).wait_recv()
        return carry

    lax.fori_loop(1, group, tk_wait, 0)
    rows8 = group * SUB
    before = (lax.broadcasted_iota(jnp.int32, (tokens, tokens), 0) < lax.broadcasted_iota(jnp.int32, (tokens, tokens), 1)).astype(F32).astype(BF16)
    row_a = lax.broadcasted_iota(jnp.int32, (rows8, rows8), 0)
    row_b = lax.broadcasted_iota(jnp.int32, (rows8, rows8), 1)
    above = jnp.logical_and(row_b < row_a, lax.div(row_b, SUB) == lax.div(row_a, SUB)).astype(F32).astype(BF16)
    row_id = lax.broadcasted_iota(jnp.int32, (rows8, tokens), 0)
    is_choice = lax.rem(row_id, SUB) < top_k

    def slots(hit):
        ones = hit.astype(F32).astype(BF16)
        upto = jnp.dot(ones, before, preferred_element_type=F32)
        rows_up = jnp.sum(jnp.dot(above, ones, preferred_element_type=F32), axis=1, keepdims=True)
        return upto + rows_up

    all_tk = tk_all[...].reshape(rows8, tokens)
    hit_in = jnp.logical_and(is_choice, lax.div(all_tk, local) == me)
    own_len = jnp.broadcast_to(tk_all[:, top_k:top_k + 1, :], (group, SUB, tokens)).reshape(rows8, tokens)
    live = jnp.logical_and(hit_in, lax.broadcasted_iota(jnp.int32, (rows8, tokens), 1) < own_len)
    slot_in[...] = jnp.where(live, slots(hit_in), -1.0).reshape(group, SUB, tokens)
    own_tk = jnp.broadcast_to(tk_ref[...][None], (group, SUB, tokens)).reshape(rows8, tokens)
    hit_out = jnp.logical_and(is_choice, lax.div(own_tk, local) == lax.div(row_id, SUB))
    slot_out[...] = jnp.where(hit_out, slots(hit_out), -1.0).reshape(group, SUB, tokens)

    keep_own.wait()
    relay(1, 1)

    slot_row = lax.broadcasted_iota(jnp.int32, (cap, tokens), 0).astype(F32)

    hops = (1, 2, 4, 3)

    def distance(c):
        return c + 1 + lax.div(c, 2) - 2 * lax.div(c, 3)

    def source(c, j):
        side = lax.div(j, 2)
        zz = zpos + (1 - side) * distance(c) - side * lax.rem(distance(c), far)
        return dev(zz, lax.rem(j, 2))

    def send_back(c, j, to):
        block = sent.at[lax.rem(c, 2), pl.ds(pl.multiple_of(j * cap, 16), cap)]
        return remote(block, back.at[me], back_s.at[c * 4 + j], back_r.at[c * 4 + lax.div(j, 2) * 2 + core], to)

    def leg_copy(way):
        j = core if way == 0 else 1 - core
        block = sent.at[0, pl.ds(pl.multiple_of(j * cap, 16), cap)]
        return remote(block, halfway.at[way], leg_s.at[way], leg_r.at[way], dev(zpos + (1 - 2 * way) * (far // 2), core))

    def fwd_copy(way):
        j = core if way == 0 else 1 - core
        sign = 1 - 2 * way
        origin = dev(zpos - sign * (far // 2), core)
        return remote(halfway.at[way], back.at[origin], fwd_s.at[way], back_r.at[8 + core], dev(zpos + sign * (far // 2), j))

    def to_sibling():
        return send_back(jnp.int32(2), 3 - core, dev(zpos, 1 - core))

    def chunk(c, carry):
        for which_c, hop in enumerate(hops):
            @pl.when(c == which_c)
            def _():
                for part in range(2):
                    for way in range(2):
                        if in_ring(way, hop, part):
                            sib_copy(way, hop, part, 1 - core).wait_recv()
                if hop == far:
                    own_copy(1 - core).wait_recv()

        def load(j):
            slot = lax.rem(j, 2)
            return pltpu.make_async_copy(rows_all.at[source(c, j)], stage.at[slot], st_sem.at[slot])

        load(jnp.int32(0)).start()

        def gather(j, inner):
            @pl.when(j < 3)
            def _():
                load(j + 1).start()

            src = source(c, j)
            pick = jnp.zeros((cap, tokens), F32)
            which = jnp.zeros((cap, tokens), F32)
            for k in range(top_k):
                same = slot_row == slot_in[src, k:k + 1, :]
                pick = jnp.where(same, 1.0, pick)
                which = jnp.where(same, lax.rem(tk_all[src, k:k + 1, :], local).astype(F32), which)
            rows = pl.ds(pl.multiple_of(j * cap, 16), cap)
            row_exp[rows, :] = jnp.broadcast_to(jnp.sum(which, axis=1, keepdims=True), (cap, LANES))
            load(j).wait()
            picked[rows, :] = jnp.dot(pick.astype(BF16), stage[lax.rem(j, 2)], preferred_element_type=F32).astype(BF16)
            return inner

        lax.fori_loop(0, 4, gather, 0)

        @pl.when(jnp.logical_and(c > 0, c < 3))
        def _():
            for j in range(4):
                send_back(c - 1, j, source(c - 1, jnp.int32(j))).start()

        @pl.when(c == 3)
        def _():
            for way in range(2):
                leg_copy(way).start()
            to_sibling().start()
            back[me] = sent[0, pl.ds(pl.multiple_of((2 + core) * cap, 16), cap), :]

        def gate_up(t, inner):
            @pl.when(t + gu_ahead < gu_tiles)
            def _():
                gu_start(False, t + gu_ahead)

            for copy in gu_copies(False, t):
                copy.wait()
            for when_c, when_t, hop, part in EVENTS:
                @pl.when(jnp.logical_and(c == when_c, t == when_t * gu_tiles // 44))
                def _():
                    relay(hop, part)

            @pl.when(jnp.logical_and(c == 3, t == HAND_ON * gu_tiles // 44))
            def _():
                for way in range(2):
                    leg_copy(way).wait_recv()
                    fwd_copy(way).start()

            both = jnp.dot(picked[...], w_gu[lax.rem(t, w_gu.shape[0])], preferred_element_type=F32)
            mixed = glu(both)
            for part in range(2):
                tile = 2 * t + part
                mine = row_exp[...] == lax.div(tile, per_exp).astype(F32)
                act[:, pl.ds(pl.multiple_of(tile * LANES, LANES), LANES)] = jnp.where(mine, mixed[:, part * LANES:(part + 1) * LANES], 0.0).astype(BF16)
            return inner

        lax.fori_loop(0, gu_tiles, gate_up, 0)

        @pl.when(c < 3)
        def _():
            prime_gu(False)

        for which_c in (2, 3):
            @pl.when(c == which_c)
            def _():
                for j in range(4):
                    before_last = jnp.int32(which_c - 2)
                    send_back(before_last, jnp.int32(j), source(before_last, jnp.int32(j))).wait_send()

        def down(t, inner):
            @pl.when(t + dn_ahead < dn_tiles)
            def _():
                dn_copy(False, t + dn_ahead).start()

            dn_copy(False, t).wait()
            out = jnp.dot(act[...], w_dn[lax.rem(t, w_dn.shape[0])], preferred_element_type=F32)
            sent[lax.rem(c, 2), :, pl.ds(pl.multiple_of(t * dn_cols, dn_cols), dn_cols)] = out.astype(BF16)
            return inner

        lax.fori_loop(0, dn_tiles, down, 0)

        @pl.when(c < 3)
        def _():
            prime_dn(False)

        return carry

    lax.fori_loop(0, 4, chunk, 0)
    for j in range(4):
        send_back(jnp.int32(3), jnp.int32(j), source(jnp.int32(3), jnp.int32(j))).start()

    def combine(i, carry):
        c = lax.div(i, 4)
        side = lax.rem(lax.div(i, 2), 2)
        zz = zpos - (1 - side) * distance(c) + side * lax.rem(distance(c), far)
        who = dev(zz, lax.rem(i, 2))

        @pl.when(i != 10 + core)
        def _():
            remote(sent.at[0, pl.ds(0, cap)], back.at[who], back_s.at[0], back_r.at[i], dev(zpos, 1 - core)).wait_recv()

        mix = jnp.zeros((cap, tokens), F32)
        for k in range(top_k):
            mix = jnp.where(slot_row == slot_out[who, k:k + 1, :], gates[k:k + 1, :], mix)
        high = mix.astype(BF16).astype(F32)
        mid = (mix - high).astype(BF16).astype(F32)
        low = mix - high - mid
        parts = jnp.transpose(jnp.concatenate([high, mid, low, jnp.zeros((three.shape[0] - 3 * cap, tokens), F32)], axis=0)).astype(BF16)
        block = back[who]
        for r in range(3):
            three[r * cap:(r + 1) * cap, :] = block

        def add(t, inner):
            cols = pl.ds(pl.multiple_of(t * 512, 512), 512)
            acc[:, cols] += jnp.dot(parts, three[:, cols], preferred_element_type=F32)
            return inner

        lax.fori_loop(0, width // 512, add, 0)
        return carry

    three[3 * cap:, :] = jnp.zeros((three.shape[0] - 3 * cap, width), BF16)
    lax.fori_loop(0, group, combine, 0)
    row = lax.broadcasted_iota(jnp.int32, (tokens, width), 0)
    y_ref[...] = jnp.where(row < len_ref[0], acc[...], 0.0).astype(BF16)

    for i in range(1, group):
        tk_copy(i, me).wait_send()
    for way in range(2):
        for hop in range(1, far + 1):
            for part in range(2):
                if in_ring(way, hop, part):
                    ring_copy(way, hop, part, True).wait_send()
                    sib_copy(way, hop, part, core).wait_send()
    own_copy(core).wait_send()
    for j in range(4):
        send_back(jnp.int32(3), jnp.int32(j), source(jnp.int32(3), jnp.int32(j))).wait_send()
    for way in range(2):
        leg_copy(way).wait_send()
        fwd_copy(way).wait_send()
    to_sibling().wait_send()


EVENTS = ((0, 16, 2, 0), (0, 40, 2, 1), (1, 4, 3, 0), (1, 24, 3, 1), (1, 43, 4, 0), (1, 43, 4, 1))
HAND_ON = 34


def moe_layer(group, u, h, topk, chunk_len, w_router, wsg, wsu, wsd, wg, wu, wd):
    tokens, width = u.shape
    top_k = topk.shape[1]
    local, _, ff = wg.shape
    shared_ff = wsg.shape[1]
    experts = w_router.shape[1]
    cap = tokens * top_k // group
    length = jnp.broadcast_to(chunk_len.reshape(1, 1), (SUB - top_k, tokens))
    tk = jnp.concatenate([topk.T, length], axis=0)
    dims = (group, tokens, width, cap, local, ff, shared_ff, top_k, experts)
    far = group // 4
    vmem = pl.BlockSpec(memory_space=pltpu.VMEM)
    hbm = pl.BlockSpec(memory_space=pl.ANY)
    smem = pl.BlockSpec(memory_space=pltpu.SMEM)
    dma = pltpu.SemaphoreType.DMA
    scratch = [
        pltpu.VMEM((group, SUB, tokens), jnp.int32),
        pltpu.VMEM((group, SUB, tokens), F32),
        pltpu.VMEM((group, SUB, tokens), F32),
        pltpu.VMEM((SUB, tokens), F32),
        pltpu.VMEM((tokens, shared_ff), BF16),
        pltpu.VMEM((4 * cap, width), BF16),
        pltpu.VMEM((4 * cap, local * ff), BF16),
        pltpu.VMEM((2, 4 * cap, width), BF16),
        pltpu.VMEM((4 * cap, LANES), F32),
        pltpu.VMEM((tokens, width), F32),
        pltpu.VMEM((3, width, 4 * LANES), BF16),
        pltpu.VMEM((3, local * ff, 256), BF16),
        pltpu.VMEM((2, tokens, width), BF16),
        pltpu.VMEM((pl.cdiv(3 * cap, 256) * 256, width), BF16),
        pltpu.VMEM((group, cap, width), BF16),
        pltpu.VMEM((2, cap, width), BF16),
        dma((group,)), dma((group,)),
        dma((2, far, 2)), dma((2, far, 2)),
        dma((2, far, 2)), dma((2, far, 2)),
        dma, dma,
        dma((group,)), dma((group,)),
        dma((2,)), dma((2,)), dma((2,)),
        dma((3, 4)), dma((3,)), dma((2,)), dma((1,)),
    ]
    return pl.pallas_call(
        functools.partial(moe_kernel, dims),
        out_shape=[jax.ShapeDtypeStruct((tokens, width), BF16), jax.ShapeDtypeStruct((group, tokens, width), BF16)],
        in_specs=[vmem, vmem, vmem, smem, vmem] + [hbm] * 6,
        out_specs=[vmem, hbm],
        scratch_shapes=scratch,
        compiler_params=pltpu.CompilerParams(collective_id=0, has_side_effects=True, vmem_limit_bytes=67043328),
    )(u, h, tk, chunk_len.reshape(1), w_router.T, wsg, wsu, wsd, wg, wu, wd.reshape(local * ff, width))[0]


def solution(mesh):
    group = mesh.shape['dpa']
    tok_spec = P(('dp', 'dpa'))
    whole = P()
    exp_spec = P('dpa')

    def device_step(x_in, chunk_len, ctx_len, lat_cache, rope_cache, topk_idx, g_attn, w_q, w_dkv, g_kv, w_kr, w_uk, w_uv, w_o, g_ffn, w_router, w_sh_gate, w_sh_up, w_sh_down, w_exp_gate, w_exp_up, w_exp_down):
        hidden, normed, lat_upd, rope_upd = attention_block(x_in[0, 0], chunk_len, ctx_len, lat_cache[0, 0], rope_cache[0, 0], g_attn, w_q, w_dkv, g_kv, w_kr, w_uk, w_uv, w_o, g_ffn)
        result = moe_layer(group, normed, hidden, topk_idx[0, 0], chunk_len, w_router, w_sh_gate, w_sh_up, w_sh_down, w_exp_gate, w_exp_up, w_exp_down)
        return result.reshape(x_in.shape), lat_upd.reshape(lat_cache.shape), rope_upd.reshape(rope_cache.shape)

    return jax.shard_map(device_step, mesh=mesh, in_specs=(tok_spec,) * 6 + (whole,) * 13 + (exp_spec,) * 3, out_specs=(tok_spec, tok_spec, tok_spec), check_vma=False)
```

```python
import functools

import jax
import jax.numpy as jnp
from jax import lax
from jax.experimental import pallas as pl
from jax.experimental.pallas import tpu as pltpu
from jax.sharding import PartitionSpec as P

EPS = 1e-6
THETA = 10000.0
MESH_ID = pl.DeviceIdType.MESH
F32 = jnp.float32
BF16 = jnp.bfloat16
LANES = 128
SUB = 8


def rms_norm(vals, gain):
    vals_f32 = vals.astype(jnp.float32)
    inv_rms = lax.rsqrt(jnp.mean(vals_f32 * vals_f32, axis=-1, keepdims=True) + EPS)
    return (vals_f32 * inv_rms * gain.astype(jnp.float32)).astype(jnp.bfloat16)


def rope_tables(positions, half):
    inv_freq = THETA ** (-2.0 * jnp.arange(half, dtype=jnp.float32) / (2 * half))
    angle = positions.astype(jnp.float32)[..., None] * inv_freq
    return jnp.cos(angle), jnp.sin(angle)


def attn_kernel(scale, len_ref, ctx_ref, x_hbm, gattn_ref, gffn_ref, gkv_ref, tab_ref, dkv_hbm, kr_hbm, q_hbm, lat_hbm, rope_hbm, uk_hbm, uv_hbm, wo_hbm, h_ref, u_ref, lat_ref, rope_ref, x, dkv, kr, q, lat_old, rope_old, uk, uv, wo, uk_wide, uv_wide, turned, lat_t, rope_rows, heads_out, sems, q_sems):
    heads, qdim, width = q.shape
    ctx_max, rank = lat_old.shape
    rope_dim = rope_old.shape[0]
    nope = qdim - rope_dim
    half = rope_dim // 2
    chunk = x.shape[0]
    copies = [pltpu.make_async_copy(src, dst, sems.at[i]) for i, (src, dst) in enumerate(((x_hbm, x), (dkv_hbm, dkv), (kr_hbm, kr), (lat_hbm, lat_old), (rope_hbm, rope_old), (uk_hbm, uk), (uv_hbm, uv), (wo_hbm, wo)))]

    def q_copy(i):
        both = pl.ds(2 * i, 2)
        return pltpu.make_async_copy(q_hbm.at[both], q.at[both], q_sems.at[i])

    for copy in copies[:5]:
        copy.start()
    for i in range(2):
        q_copy(i).start()
    for copy in copies[5:7]:
        copy.start()
    for i in range(2, heads // 2):
        q_copy(i).start()
    copies[7].start()
    clen = len_ref[0]
    ctx = ctx_ref[0]
    cos_tab = tab_ref[:half, :]
    sin_tab = tab_ref[half:, :]

    def roped(vals):
        first = vals[:half]
        second = vals[half:]
        return jnp.concatenate([first * cos_tab - second * sin_tab, second * cos_tab + first * sin_tab], axis=0).astype(BF16)

    def normed(vals, gain_ref):
        gain = gain_ref[...].astype(F32).reshape(1, gain_ref.shape[0])
        return vals * lax.rsqrt(jnp.mean(vals * vals, axis=1, keepdims=True) + EPS) * gain

    copies[0].wait()
    a = normed(x[...].astype(F32), gattn_ref).astype(BF16)
    turned[...] = jnp.transpose(a.astype(F32)).astype(BF16)
    copies[1].wait()
    lat_new = normed(jnp.dot(a, dkv[...], preferred_element_type=F32), gkv_ref).astype(BF16)
    copies[2].wait()
    rope_new = roped(jnp.dot(kr[...], turned[...], preferred_element_type=F32))
    place = lax.broadcasted_iota(jnp.int32, (ctx_max, chunk), 0) - ctx
    row = lax.broadcasted_iota(jnp.int32, (ctx_max, chunk), 1)
    move = jnp.where(jnp.logical_and(place == row, row < clen), 1.0, 0.0).astype(BF16)
    pos = lax.broadcasted_iota(jnp.int32, (ctx_max, rank), 0) - ctx
    copies[3].wait()
    lat = jnp.where(jnp.logical_and(pos >= 0, pos < clen), jnp.dot(move, lat_new, preferred_element_type=F32), lat_old[...].astype(F32))
    lat_ref[...] = lat.astype(BF16)
    lat_t[...] = jnp.transpose(lat).astype(BF16)
    place = lax.broadcasted_iota(jnp.int32, (chunk, ctx_max), 1) - ctx
    row = lax.broadcasted_iota(jnp.int32, (chunk, ctx_max), 0)
    move = jnp.where(jnp.logical_and(place == row, row < clen), 1.0, 0.0).astype(BF16)
    pos = lax.broadcasted_iota(jnp.int32, (rope_dim, ctx_max), 1) - ctx
    copies[4].wait()
    rope = jnp.where(jnp.logical_and(pos >= 0, pos < clen), jnp.dot(rope_new, move, preferred_element_type=F32), rope_old[...].astype(F32))
    rope_ref[...] = rope.astype(BF16)
    rope_rows[...] = jnp.transpose(jnp.concatenate([rope, jnp.zeros_like(rope)], axis=0)).astype(BF16)
    copies[5].wait()
    uk_wide[...] = uk[...].astype(F32)
    copies[6].wait()
    uv_wide[...] = uv[...].astype(F32)
    seen = lax.broadcasted_iota(jnp.int32, (ctx_max, chunk), 0) - lax.broadcasted_iota(jnp.int32, (ctx_max, chunk), 1) <= ctx
    factor = scale * 1.4426950408889634

    def pair(i, carry):
        q_copy(i).wait()
        both = jnp.dot(q[pl.ds(2 * i, 2)].reshape(2 * qdim, width), turned[...], preferred_element_type=F32).astype(BF16)
        lats = []
        ropes = []
        for k in range(2):
            mine = both[k * qdim:(k + 1) * qdim]
            up = uk_wide[pl.ds(2 * i + k, rank, stride=heads), :].astype(BF16)
            lats.append(jnp.dot(up, mine[:nope], preferred_element_type=F32).astype(BF16))
            ropes.append(roped(mine[nope:].astype(F32)))
        ropes = jnp.concatenate(ropes, axis=1)
        scores = jnp.dot(lat_ref[...], jnp.concatenate(lats, axis=1), preferred_element_type=F32) + jnp.dot(rope_rows[:, :rope_dim], ropes, preferred_element_type=F32)
        probs = []
        for k in range(2):
            mine = jnp.where(seen, scores[:, k * chunk:(k + 1) * chunk], -1e30)
            weight = jnp.exp2((mine - jnp.max(mine, axis=0, keepdims=True)) * factor)
            probs.append((weight * (1.0 / jnp.sum(weight, axis=0, keepdims=True))).astype(BF16))
        out = jnp.dot(lat_t[...], jnp.concatenate(probs, axis=1), preferred_element_type=F32).astype(BF16)
        for k in range(2):
            up = uv_wide[pl.ds(2 * i + k, rank, stride=heads), :].astype(BF16)
            mine = lax.dot_general(out[:, k * chunk:(k + 1) * chunk], up, (((0,), (0,)), ((), ())), preferred_element_type=F32)
            heads_out[:, pl.ds(pl.multiple_of((2 * i + k) * nope, nope), nope)] = mine.astype(BF16)
        return carry

    lax.fori_loop(0, heads // 2, pair, 0)
    copies[7].wait()

    def project(t, total):
        cols = pl.ds(pl.multiple_of(t * 256, 256), 256)
        out = jnp.dot(heads_out[...], wo[:, cols], preferred_element_type=F32).astype(BF16)
        hidden = (x[:, cols].astype(F32) + out.astype(F32)).astype(BF16)
        h_ref[:, cols] = hidden
        wide_h = hidden.astype(F32)
        return total + jnp.sum(wide_h * wide_h, axis=1, keepdims=True)

    total = lax.fori_loop(0, width // 256, project, jnp.zeros((chunk, 1), F32))
    inv = lax.rsqrt(total / width + EPS)
    gain = gffn_ref[...].astype(F32).reshape(1, width)
    u_ref[...] = (h_ref[...].astype(F32) * inv * gain).astype(BF16)


def attention_block(x, chunk_len, ctx_len, lat_cache, rope_cache, g_attn, w_q, w_dkv, g_kv, w_kr, w_uk, w_uv, w_o, g_ffn):
    chunk, width = x.shape
    ctx_max, rank = lat_cache.shape
    rope_dim = rope_cache.shape[1]
    heads, qdim = w_q.shape[1:]
    nope = qdim - rope_dim
    vdim = w_uv.shape[2]
    tab = jnp.concatenate(rope_tables(ctx_len.reshape(1) + jnp.arange(chunk), rope_dim // 2), axis=1).T
    vmem = pl.BlockSpec(memory_space=pltpu.VMEM)
    hbm = pl.BlockSpec(memory_space=pl.ANY)
    smem = pl.BlockSpec(memory_space=pltpu.SMEM)
    low = [(chunk, width), (width, rank), (rope_dim, width), (heads, qdim, width), (ctx_max, rank), (rope_dim, ctx_max), (rank * heads, nope), (rank * heads, vdim), (heads * vdim, width)]
    wide = [(rank * heads, nope), (rank * heads, vdim)]
    more = [(width, chunk), (rank, ctx_max), (ctx_max, 2 * rope_dim), (chunk, heads * vdim)]
    hidden, normed, lat, rope = pl.pallas_call(
        functools.partial(attn_kernel, qdim ** -0.5),
        out_shape=[jax.ShapeDtypeStruct((chunk, width), BF16), jax.ShapeDtypeStruct((chunk, width), BF16), jax.ShapeDtypeStruct((ctx_max, rank), BF16), jax.ShapeDtypeStruct((rope_dim, ctx_max), BF16)],
        in_specs=[smem, smem, hbm, vmem, vmem, vmem, vmem] + [hbm] * 8,
        out_specs=[vmem] * 4,
        scratch_shapes=[pltpu.VMEM(shape, BF16) for shape in low] + [pltpu.VMEM(shape, F32) for shape in wide] + [pltpu.VMEM(shape, BF16) for shape in more] + [pltpu.SemaphoreType.DMA((8,)), pltpu.SemaphoreType.DMA((heads // 2,))],
        compiler_params=pltpu.CompilerParams(vmem_limit_bytes=67043328),
    )(chunk_len.reshape(1), ctx_len.reshape(1), x, g_attn, g_ffn, g_kv, tab, w_dkv, w_kr.T, w_q.transpose(1, 2, 0), lat_cache, rope_cache.T, w_uk.reshape(rank * heads, nope), w_uv.reshape(rank * heads, vdim), w_o.reshape(heads * vdim, width))
    return hidden, normed, lat, rope.T


def moe_kernel(dims, u_ref, h_ref, tk_ref, len_ref, wr_ref, wsg, wsu, wsd, wg, wu, wd, y_ref, rows_all, tk_all, slot_in, slot_out, gates, sh_act, picked, act, sent, row_exp, acc, w_gu, w_dn, stage, three, back, halfway, tk_s, tk_r, ring_s, ring_r, sib_s, sib_r, own_s, own_r, back_s, back_r, leg_s, leg_r, fwd_s, gu_sem, dn_sem, st_sem, loc_sem):
    group, tokens, width, cap, local, ff, shared_ff, top_k, experts = dims
    ring = group // 2
    half = tokens // 2
    chunk_rows = 4 * cap
    gu_tiles = local * ff // (2 * LANES)
    per_exp = ff // LANES
    sh_tiles = shared_ff // (2 * LANES)
    dn_cols = w_dn.shape[2]
    dn_tiles = width // dn_cols
    me = lax.axis_index('dpa')
    zpos = lax.div(me, 2)
    core = lax.rem(me, 2)

    def dev(zz, cc):
        return lax.rem(zz + 2 * ring, ring) * 2 + cc

    def remote(src, dst, s_sem, r_sem, to):
        return pltpu.make_async_remote_copy(src_ref=src, dst_ref=dst, send_sem=s_sem, recv_sem=r_sem, device_id={'dpa': to}, device_id_type=MESH_ID)

    barrier = pltpu.get_barrier_semaphore()

    def greet(i, carry):
        pl.semaphore_signal(barrier, inc=1, device_id={'dpa': lax.rem(me + i, group)}, device_id_type=MESH_ID)
        return carry

    lax.fori_loop(1, group, greet, 0)
    pl.semaphore_wait(barrier, group - 1)

    def tk_copy(i, owner):
        return remote(tk_ref, tk_all.at[owner], tk_s.at[i], tk_r.at[i], lax.rem(me + i, group))

    def tk_start(i, carry):
        tk_copy(i, me).start()
        return carry

    lax.fori_loop(1, group, tk_start, 0)

    def ring_copy(way, hop, part, sending):
        sign = 1 - 2 * way
        owner = dev(zpos - sign * (hop - 1 if sending else hop), core)
        rows = pl.ds(part * half, half)
        dst = rows_all.at[owner, rows]
        src = u_ref.at[rows] if sending and hop == 1 else dst
        return remote(src, dst, ring_s.at[way, hop - 1, part], ring_r.at[way, hop - 1, part], dev(zpos + sign, core))

    def sib_copy(way, hop, part, cc):
        sign = 1 - 2 * way
        block = rows_all.at[dev(zpos - sign * hop, cc), pl.ds(part * half, half)]
        return remote(block, block, sib_s.at[way, hop - 1, part], sib_r.at[way, hop - 1, part], dev(zpos, 1 - core))

    far = ring // 2

    def in_ring(way, hop, part):
        return hop < far or (hop == far and part == way)

    def own_copy(cc):
        return remote(u_ref, rows_all.at[dev(zpos, cc)], own_s, own_r, dev(zpos, 1 - core))

    keep_own = pltpu.make_async_copy(u_ref, rows_all.at[me], loc_sem.at[0])
    for part in range(2):
        for way in range(2):
            ring_copy(way, 1, part, True).start()
    own_copy(core).start()
    keep_own.start()

    def relay(hop, part):
        for way in range(2):
            if in_ring(way, hop, part):
                ring_copy(way, hop, part, False).wait_recv()
                if in_ring(way, hop + 1, part):
                    ring_copy(way, hop + 1, part, True).start()
                sib_copy(way, hop, part, core).start()

    def gu_copies(shared, t):
        slot = lax.rem(t, w_gu.shape[0])
        if shared:
            cols = pl.ds(pl.multiple_of(t * 2 * LANES, 2 * LANES), 2 * LANES)
            srcs = (wsg.at[:, cols], wsu.at[:, cols])
        else:
            srcs = []
            for ref in (wg, wu):
                for part in range(2):
                    tile = 2 * t + part
                    cols = pl.ds(pl.multiple_of(lax.rem(tile, per_exp) * LANES, LANES), LANES)
                    srcs.append(ref.at[lax.div(tile, per_exp), :, cols])
        span = 4 * LANES // len(srcs)
        return [pltpu.make_async_copy(src, w_gu.at[slot, :, pl.ds(i * span, span)], gu_sem.at[slot, i]) for i, src in enumerate(srcs)]

    def dn_copy(shared, t):
        slot = lax.rem(t, w_dn.shape[0])
        cols = pl.ds(pl.multiple_of(t * dn_cols, dn_cols), dn_cols)
        if shared:
            return pltpu.make_async_copy(wsd.at[:, cols], w_dn.at[slot, pl.ds(0, shared_ff)], dn_sem.at[slot])
        return pltpu.make_async_copy(wd.at[:, cols], w_dn.at[slot], dn_sem.at[slot])

    gu_ahead = w_gu.shape[0] - 1
    dn_ahead = w_dn.shape[0] - 1

    def gu_start(shared, t):
        for copy in gu_copies(shared, t):
            copy.start()

    def prime_gu(shared):
        for t in range(gu_ahead):
            gu_start(shared, jnp.int32(t))

    def prime_dn(shared):
        for t in range(dn_ahead):
            dn_copy(shared, jnp.int32(t)).start()

    prime_gu(True)
    prime_dn(True)

    logits = lax.dot_general(wr_ref[...], u_ref[...], (((1,), (1,)), ((), ())), preferred_element_type=F32)
    shifted = jnp.exp(logits - jnp.max(logits, axis=0, keepdims=True))
    prob = shifted / jnp.sum(shifted, axis=0, keepdims=True)
    exp_row = lax.broadcasted_iota(jnp.int32, (experts, tokens), 0)
    for k in range(SUB):
        if k < top_k:
            gates[k:k + 1, :] = jnp.sum(jnp.where(exp_row == tk_ref[k:k + 1, :], prob, 0.0), axis=0, keepdims=True)
        else:
            gates[k:k + 1, :] = jnp.zeros((1, tokens), F32)

    def glu(both):
        gate = both[:, :2 * LANES]
        return gate * jax.nn.sigmoid(gate) * both[:, 2 * LANES:]

    def sh_gu(t, carry):
        @pl.when(t + gu_ahead < sh_tiles)
        def _():
            gu_start(True, t + gu_ahead)

        for copy in gu_copies(True, t):
            copy.wait()
        both = jnp.dot(u_ref[...], w_gu[lax.rem(t, w_gu.shape[0])], preferred_element_type=F32)
        sh_act[:, pl.ds(pl.multiple_of(t * 2 * LANES, 2 * LANES), 2 * LANES)] = glu(both).astype(BF16)
        return carry

    lax.fori_loop(0, sh_tiles, sh_gu, 0)
    prime_gu(False)
    relay(1, 0)

    def sh_dn(t, carry):
        @pl.when(t + dn_ahead < dn_tiles)
        def _():
            dn_copy(True, t + dn_ahead).start()

        dn_copy(True, t).wait()
        cols = pl.ds(pl.multiple_of(t * dn_cols, dn_cols), dn_cols)
        tile = w_dn[lax.rem(t, w_dn.shape[0]), :shared_ff]
        acc[:, cols] = h_ref[:, cols].astype(F32) + jnp.dot(sh_act[...], tile, preferred_element_type=F32)
        return carry

    lax.fori_loop(0, dn_tiles, sh_dn, 0)
    prime_dn(False)

    tk_all[me] = tk_ref[...]

    def tk_wait(i, carry):
        tk_copy(i, lax.rem(me - i + group, group)).wait_recv()
        return carry

    lax.fori_loop(1, group, tk_wait, 0)
    rows8 = group * SUB
    before = (lax.broadcasted_iota(jnp.int32, (tokens, tokens), 0) < lax.broadcasted_iota(jnp.int32, (tokens, tokens), 1)).astype(F32).astype(BF16)
    row_a = lax.broadcasted_iota(jnp.int32, (rows8, rows8), 0)
    row_b = lax.broadcasted_iota(jnp.int32, (rows8, rows8), 1)
    above = jnp.logical_and(row_b < row_a, lax.div(row_b, SUB) == lax.div(row_a, SUB)).astype(F32).astype(BF16)
    row_id = lax.broadcasted_iota(jnp.int32, (rows8, tokens), 0)
    is_choice = lax.rem(row_id, SUB) < top_k

    def slots(hit):
        ones = hit.astype(F32).astype(BF16)
        upto = jnp.dot(ones, before, preferred_element_type=F32)
        rows_up = jnp.sum(jnp.dot(above, ones, preferred_element_type=F32), axis=1, keepdims=True)
        return upto + rows_up

    all_tk = tk_all[...].reshape(rows8, tokens)
    hit_in = jnp.logical_and(is_choice, lax.div(all_tk, local) == me)
    own_len = jnp.broadcast_to(tk_all[:, top_k:top_k + 1, :], (group, SUB, tokens)).reshape(rows8, tokens)
    live = jnp.logical_and(hit_in, lax.broadcasted_iota(jnp.int32, (rows8, tokens), 1) < own_len)
    slot_in[...] = jnp.where(live, slots(hit_in), -1.0).reshape(group, SUB, tokens)
    own_tk = jnp.broadcast_to(tk_ref[...][None], (group, SUB, tokens)).reshape(rows8, tokens)
    hit_out = jnp.logical_and(is_choice, lax.div(own_tk, local) == lax.div(row_id, SUB))
    slot_out[...] = jnp.where(hit_out, slots(hit_out), -1.0).reshape(group, SUB, tokens)

    keep_own.wait()
    relay(1, 1)

    slot_row = lax.broadcasted_iota(jnp.int32, (cap, tokens), 0).astype(F32)

    hops = (1, 2, 4, 3)

    def distance(c):
        return c + 1 + lax.div(c, 2) - 2 * lax.div(c, 3)

    def source(c, j):
        side = lax.div(j, 2)
        zz = zpos + (1 - side) * distance(c) - side * lax.rem(distance(c), far)
        return dev(zz, lax.rem(j, 2))

    def send_back(c, j, to):
        block = sent.at[lax.rem(c, 2), pl.ds(pl.multiple_of(j * cap, 16), cap)]
        return remote(block, back.at[me], back_s.at[c * 4 + j], back_r.at[c * 4 + lax.div(j, 2) * 2 + core], to)

    def leg_copy(way):
        j = core if way == 0 else 1 - core
        block = sent.at[0, pl.ds(pl.multiple_of(j * cap, 16), cap)]
        return remote(block, halfway.at[way], leg_s.at[way], leg_r.at[way], dev(zpos + (1 - 2 * way) * (far // 2), core))

    def fwd_copy(way):
        j = core if way == 0 else 1 - core
        sign = 1 - 2 * way
        origin = dev(zpos - sign * (far // 2), core)
        return remote(halfway.at[way], back.at[origin], fwd_s.at[way], back_r.at[8 + core], dev(zpos + sign * (far // 2), j))

    def to_sibling():
        return send_back(jnp.int32(2), 3 - core, dev(zpos, 1 - core))

    def chunk(c, carry):
        for which_c, hop in enumerate(hops):
            @pl.when(c == which_c)
            def _():
                for part in range(2):
                    for way in range(2):
                        if in_ring(way, hop, part):
                            sib_copy(way, hop, part, 1 - core).wait_recv()
                if hop == far:
                    own_copy(1 - core).wait_recv()

        def load(j):
            slot = lax.rem(j, 2)
            return pltpu.make_async_copy(rows_all.at[source(c, j)], stage.at[slot], st_sem.at[slot])

        load(jnp.int32(0)).start()

        def gather(j, inner):
            @pl.when(j < 3)
            def _():
                load(j + 1).start()

            src = source(c, j)
            pick = jnp.zeros((cap, tokens), F32)
            which = jnp.zeros((cap, tokens), F32)
            for k in range(top_k):
                same = slot_row == slot_in[src, k:k + 1, :]
                pick = jnp.where(same, 1.0, pick)
                which = jnp.where(same, lax.rem(tk_all[src, k:k + 1, :], local).astype(F32), which)
            rows = pl.ds(pl.multiple_of(j * cap, 16), cap)
            row_exp[rows, :] = jnp.broadcast_to(jnp.sum(which, axis=1, keepdims=True), (cap, LANES))
            load(j).wait()
            picked[rows, :] = jnp.dot(pick.astype(BF16), stage[lax.rem(j, 2)], preferred_element_type=F32).astype(BF16)
            return inner

        lax.fori_loop(0, 4, gather, 0)

        @pl.when(c == 2)
        def _():
            for j in range(4):
                send_back(c - 1, j, source(c - 1, jnp.int32(j))).start()

        @pl.when(c == 3)
        def _():
            for way in range(2):
                leg_copy(way).start()
            to_sibling().start()
            back[me] = sent[0, pl.ds(pl.multiple_of((2 + core) * cap, 16), cap), :]

        def gate_up(t, inner):
            @pl.when(t + gu_ahead < gu_tiles)
            def _():
                gu_start(False, t + gu_ahead)

            for copy in gu_copies(False, t):
                copy.wait()
            for when_c, when_t, hop, part in EVENTS:
                @pl.when(jnp.logical_and(c == when_c, t == when_t * gu_tiles // 44))
                def _():
                    relay(hop, part)

            @pl.when(jnp.logical_and(c == 1, t == SEND_FIRST * gu_tiles // 44))
            def _():
                for j in range(4):
                    send_back(c - 1, j, source(c - 1, jnp.int32(j))).start()

            @pl.when(jnp.logical_and(c == 3, t == HAND_ON * gu_tiles // 44))
            def _():
                for way in range(2):
                    leg_copy(way).wait_recv()
                    fwd_copy(way).start()

            both = jnp.dot(picked[...], w_gu[lax.rem(t, w_gu.shape[0])], preferred_element_type=F32)
            mixed = glu(both)
            for part in range(2):
                tile = 2 * t + part
                mine = row_exp[...] == lax.div(tile, per_exp).astype(F32)
                act[:, pl.ds(pl.multiple_of(tile * LANES, LANES), LANES)] = jnp.where(mine, mixed[:, part * LANES:(part + 1) * LANES], 0.0).astype(BF16)
            return inner

        lax.fori_loop(0, gu_tiles, gate_up, 0)

        @pl.when(c < 3)
        def _():
            prime_gu(False)

        for which_c in (2, 3):
            @pl.when(c == which_c)
            def _():
                for j in range(4):
                    before_last = jnp.int32(which_c - 2)
                    send_back(before_last, jnp.int32(j), source(before_last, jnp.int32(j))).wait_send()

        def down(t, inner):
            @pl.when(t + dn_ahead < dn_tiles)
            def _():
                dn_copy(False, t + dn_ahead).start()

            dn_copy(False, t).wait()
            out = jnp.dot(act[...], w_dn[lax.rem(t, w_dn.shape[0])], preferred_element_type=F32)
            sent[lax.rem(c, 2), :, pl.ds(pl.multiple_of(t * dn_cols, dn_cols), dn_cols)] = out.astype(BF16)
            return inner

        lax.fori_loop(0, dn_tiles, down, 0)

        @pl.when(c < 3)
        def _():
            prime_dn(False)

        return carry

    lax.fori_loop(0, 4, chunk, 0)
    for j in (0, 1, 3, 2):
        send_back(jnp.int32(3), jnp.int32(j), source(jnp.int32(3), jnp.int32(j))).start()

    def combine(i, carry):
        c = lax.div(i, 4)
        side = lax.rem(lax.div(i, 2) + core * lax.div(c, 3), 2)
        at = 4 * c + 2 * side + lax.rem(i, 2)
        zz = zpos - (1 - side) * distance(c) + side * lax.rem(distance(c), far)
        who = dev(zz, lax.rem(i, 2))

        @pl.when(at != 10 + core)
        def _():
            remote(sent.at[0, pl.ds(0, cap)], back.at[who], back_s.at[0], back_r.at[at], dev(zpos, 1 - core)).wait_recv()

        mix = jnp.zeros((cap, tokens), F32)
        for k in range(top_k):
            mix = jnp.where(slot_row == slot_out[who, k:k + 1, :], gates[k:k + 1, :], mix)
        high = mix.astype(BF16).astype(F32)
        mid = (mix - high).astype(BF16).astype(F32)
        low = mix - high - mid
        parts = jnp.transpose(jnp.concatenate([high, mid, low, jnp.zeros((three.shape[0] - 3 * cap, tokens), F32)], axis=0)).astype(BF16)
        block = back[who]
        for r in range(3):
            three[r * cap:(r + 1) * cap, :] = block

        def add(t, inner):
            cols = pl.ds(pl.multiple_of(t * 512, 512), 512)
            acc[:, cols] += jnp.dot(parts, three[:, cols], preferred_element_type=F32)
            return inner

        lax.fori_loop(0, width // 512, add, 0)
        return carry

    three[3 * cap:, :] = jnp.zeros((three.shape[0] - 3 * cap, width), BF16)
    lax.fori_loop(0, group, combine, 0)
    row = lax.broadcasted_iota(jnp.int32, (tokens, width), 0)
    y_ref[...] = jnp.where(row < len_ref[0], acc[...], 0.0).astype(BF16)

    for i in range(1, group):
        tk_copy(i, me).wait_send()
    for way in range(2):
        for hop in range(1, far + 1):
            for part in range(2):
                if in_ring(way, hop, part):
                    ring_copy(way, hop, part, True).wait_send()
                    sib_copy(way, hop, part, core).wait_send()
    own_copy(core).wait_send()
    for j in range(4):
        send_back(jnp.int32(3), jnp.int32(j), source(jnp.int32(3), jnp.int32(j))).wait_send()
    for way in range(2):
        leg_copy(way).wait_send()
        fwd_copy(way).wait_send()
    to_sibling().wait_send()


EVENTS = ((0, 16, 2, 0), (0, 40, 2, 1), (1, 4, 3, 0), (1, 20, 3, 1), (1, 43, 4, 0), (1, 43, 4, 1))
SEND_FIRST = 26
HAND_ON = 40


def moe_layer(group, u, h, topk, chunk_len, w_router, wsg, wsu, wsd, wg, wu, wd):
    tokens, width = u.shape
    top_k = topk.shape[1]
    local, _, ff = wg.shape
    shared_ff = wsg.shape[1]
    experts = w_router.shape[1]
    cap = tokens * top_k // group
    length = jnp.broadcast_to(chunk_len.reshape(1, 1), (SUB - top_k, tokens))
    tk = jnp.concatenate([topk.T, length], axis=0)
    dims = (group, tokens, width, cap, local, ff, shared_ff, top_k, experts)
    far = group // 4
    vmem = pl.BlockSpec(memory_space=pltpu.VMEM)
    hbm = pl.BlockSpec(memory_space=pl.ANY)
    smem = pl.BlockSpec(memory_space=pltpu.SMEM)
    dma = pltpu.SemaphoreType.DMA
    scratch = [
        pltpu.VMEM((group, SUB, tokens), jnp.int32),
        pltpu.VMEM((group, SUB, tokens), F32),
        pltpu.VMEM((group, SUB, tokens), F32),
        pltpu.VMEM((SUB, tokens), F32),
        pltpu.VMEM((tokens, shared_ff), BF16),
        pltpu.VMEM((4 * cap, width), BF16),
        pltpu.VMEM((4 * cap, local * ff), BF16),
        pltpu.VMEM((2, 4 * cap, width), BF16),
        pltpu.VMEM((4 * cap, LANES), F32),
        pltpu.VMEM((tokens, width), F32),
        pltpu.VMEM((3, width, 4 * LANES), BF16),
        pltpu.VMEM((3, local * ff, 256), BF16),
        pltpu.VMEM((2, tokens, width), BF16),
        pltpu.VMEM((pl.cdiv(3 * cap, 256) * 256, width), BF16),
        pltpu.VMEM((group, cap, width), BF16),
        pltpu.VMEM((2, cap, width), BF16),
        dma((group,)), dma((group,)),
        dma((2, far, 2)), dma((2, far, 2)),
        dma((2, far, 2)), dma((2, far, 2)),
        dma, dma,
        dma((group,)), dma((group,)),
        dma((2,)), dma((2,)), dma((2,)),
        dma((3, 4)), dma((3,)), dma((2,)), dma((1,)),
    ]
    return pl.pallas_call(
        functools.partial(moe_kernel, dims),
        out_shape=[jax.ShapeDtypeStruct((tokens, width), BF16), jax.ShapeDtypeStruct((group, tokens, width), BF16)],
        in_specs=[vmem, vmem, vmem, smem, vmem] + [hbm] * 6,
        out_specs=[vmem, hbm],
        scratch_shapes=scratch,
        compiler_params=pltpu.CompilerParams(collective_id=0, has_side_effects=True, vmem_limit_bytes=67043328),
    )(u, h, tk, chunk_len.reshape(1), w_router.T, wsg, wsu, wsd, wg, wu, wd.reshape(local * ff, width))[0]


def solution(mesh):
    group = mesh.shape['dpa']
    tok_spec = P(('dp', 'dpa'))
    whole = P()
    exp_spec = P('dpa')

    def device_step(x_in, chunk_len, ctx_len, lat_cache, rope_cache, topk_idx, g_attn, w_q, w_dkv, g_kv, w_kr, w_uk, w_uv, w_o, g_ffn, w_router, w_sh_gate, w_sh_up, w_sh_down, w_exp_gate, w_exp_up, w_exp_down):
        hidden, normed, lat_upd, rope_upd = attention_block(x_in[0, 0], chunk_len, ctx_len, lat_cache[0, 0], rope_cache[0, 0], g_attn, w_q, w_dkv, g_kv, w_kr, w_uk, w_uv, w_o, g_ffn)
        result = moe_layer(group, normed, hidden, topk_idx[0, 0], chunk_len, w_router, w_sh_gate, w_sh_up, w_sh_down, w_exp_gate, w_exp_up, w_exp_down)
        return result.reshape(x_in.shape), lat_upd.reshape(lat_cache.shape), rope_upd.reshape(rope_cache.shape)

    return jax.shard_map(device_step, mesh=mesh, in_specs=(tok_spec,) * 6 + (whole,) * 13 + (exp_spec,) * 3, out_specs=(tok_spec, tok_spec, tok_spec), check_vma=False)
```
